32 devices in a mesh: inner: 4 (over y, x), wide: 8 (over z, core).
Axes of the slice: x: 2, y: 2, z: 4, core: 2. Of those that a mesh axis runs over, the one named last changes fastest.
Arguments:
- response: float32 [65536, 512], P(('inner', 'wide')), as said below
Outputs:
- upper_factor: float32 [512, 512], replicated
- q_rows: float32 [65536, 512], P(('inner', 'wide'))
Inputs may be any that keep to these rules, and one draw needn't show every extreme that they name: `response`: real and imaginary parts of measured receiver responses; the panel has full column rank.
All inputs are finite; a program needn't handle non-finite values.
Results may differ from the reference program's by a relative error of at most 0.0001.
Values sent between devices are 32-bit elements; how exact they have to be, the bound alone decides.
No kernel may reach another device: no remote copies, remote signals or barrier semaphores. Data moves between devices by JAX's collectives and lax.ppermute only.
A program may use at most 128 MiB of HBM per device.

```python
import math
import jax
import jax.numpy as jnp
from jax import lax

W = 512
ROWS_DEV = 2048
ROWS = 65536


def draw_response(key, part):
    key_values, key_rows, key_cols = jax.random.split(key, 3)
    position = jnp.arange(ROWS, dtype=jnp.float32) / ROWS
    trend = jnp.exp(math.log(3.0) * position)[:, None]
    col_scale = jnp.exp(jax.random.uniform(key_cols, (1, W), jnp.float32, 0.0, math.log(10.0)))
    values = jax.random.truncated_normal(key_values, -6.0, 6.0, (ROWS, W), jnp.float32)
    row_rough = jnp.exp(jax.random.uniform(key_rows, (ROWS, 1), jnp.float32, 0.0, math.log(10.0)))
    return (values * row_rough * trend * col_scale * 0.25).astype(jnp.float32)


def setup_inputs(seed: int = 0) -> dict:
    keys = jax.random.split(jax.random.key(seed), 2)
    return {
        "response": draw_response(jax.random.fold_in(keys[1], 71), 0),
    }


def reference(response):
    blocks = response.reshape(ROWS // ROWS_DEV, ROWS_DEV, W)

    def accumulate(running, block_rows):
        part_gram = lax.dot_general(block_rows.astype(jnp.float32), block_rows.astype(jnp.float32), (((0,), (0,)), ((), ())), precision=lax.Precision.HIGHEST, preferred_element_type=jnp.float32)
        return (running + part_gram, None)
    gram_matrix, unused = lax.scan(accumulate, jnp.zeros((W, W), jnp.float32), blocks)
    gram_matrix = gram_matrix / ROWS
    lower_factor = jnp.linalg.cholesky(gram_matrix)

    def solve_block(block_rows):
        return jax.scipy.linalg.solve_triangular(lower_factor, block_rows.T, lower=True).T
    q_rows = lax.map(solve_block, blocks).reshape(ROWS, W)
    return (lower_factor.T, q_rows)
```

```python
import jax
import jax.numpy as jnp
from jax import lax
from jax.sharding import PartitionSpec as P

base_width = 128


def matmul(left, right):
    return jnp.dot(left, right, precision=lax.Precision.HIGHEST, preferred_element_type=jnp.float32)


def gram_of(matrix):
    return lax.dot_general(
        matrix,
        matrix,
        (((0,), (0,)), ((), ())),
        precision=lax.Precision.HIGHEST,
        preferred_element_type=jnp.float32,
    )


def lower_inverse(lower):
    width = lower.shape[0]
    if width <= base_width:
        diag_part = jnp.diagonal(lower)
        unit_lower = lower / diag_part[:, None]
        strict = jnp.eye(width, dtype=jnp.float32) - unit_lower
        result = jnp.eye(width, dtype=jnp.float32) + strict
        power = strict
        reach = 2
        while reach < width:
            power = matmul(power, power)
            result = result + matmul(result, power)
            reach = reach * 2
        return result / diag_part[None, :]
    half = width // 2
    first_inv = lower_inverse(lower[:half, :half])
    second_inv = lower_inverse(lower[half:, half:])
    corner = -matmul(second_inv, matmul(lower[half:, :half], first_inv))
    top = jnp.concatenate([first_inv, jnp.zeros((half, width - half), jnp.float32)], axis=1)
    bottom = jnp.concatenate([corner, second_inv], axis=1)
    return jnp.concatenate([top, bottom], axis=0)


def lower_cholesky(gram_matrix):
    width = gram_matrix.shape[0]
    if width <= base_width:
        return jnp.linalg.cholesky(gram_matrix)
    half = width // 2
    first = lower_cholesky(gram_matrix[:half, :half])
    first_inv = lower_inverse(first)
    below = matmul(gram_matrix[half:, :half], first_inv.T)
    second = lower_cholesky(gram_matrix[half:, half:] - matmul(below, below.T))
    top = jnp.concatenate([first, jnp.zeros((half, width - half), jnp.float32)], axis=1)
    bottom = jnp.concatenate([below, second], axis=1)
    return jnp.concatenate([top, bottom], axis=0)


def upper_of(gram_matrix):
    return lower_cholesky(gram_matrix).T


def group_index(axis, shift, size):
    return (lax.axis_index(axis) >> shift) & (size - 1)


def partner_xor(value, axis, shift, offset):
    mask = offset << shift
    pairs = [(source, source ^ mask) for source in range(lax.axis_size(axis))]
    return lax.ppermute(value, axis, pairs)


def scatter_sum(value, axis, shift, size):
    height = value.shape[0] // size
    index = group_index(axis, shift, size)
    chunk = lambda j: lax.dynamic_slice_in_dim(value, j * height, height, 0)
    total = chunk(index)
    for offset in range(1, size):
        total = total + partner_xor(chunk(index ^ offset), axis, shift, offset)
    return total


def gather_all(chunk, axis, shift, size):
    height = chunk.shape[0]
    index = group_index(axis, shift, size)
    whole = jnp.zeros((height * size, chunk.shape[1]), chunk.dtype)
    whole = lax.dynamic_update_slice_in_dim(whole, chunk, index * height, 0)
    for offset in range(1, size):
        got = partner_xor(chunk, axis, shift, offset)
        whole = lax.dynamic_update_slice_in_dim(whole, got, (index ^ offset) * height, 0)
    return whole


def axis_groups(axis, first):
    bits = lax.axis_size(axis).bit_length() - 1
    groups = []
    shift = first
    while shift < bits:
        width = min(2, bits - shift)
        groups.append((axis, shift, 2**width))
        shift += width
    return groups


def all_sum(gram_matrix):
    groups = [("wide", 0, 2)] + axis_groups("inner", 0) + axis_groups("wide", 1)
    for group in groups:
        gram_matrix = scatter_sum(gram_matrix, *group)
    for group in reversed(groups):
        gram_matrix = gather_all(gram_matrix, *group)
    return gram_matrix


def on_device(response):
    row_count = response.shape[0] * lax.axis_size("inner") * lax.axis_size("wide")
    gram_matrix = gram_of(response) / row_count
    gram_matrix = all_sum(gram_matrix)
    upper_factor = upper_of(gram_matrix)
    inverse_lower = lower_inverse(upper_factor.T)
    q_rows = matmul(response, inverse_lower.T)
    return (upper_factor, q_rows)


def solution(mesh):
    in_specs = (P(("inner", "wide"), None),)
    out_specs = (P(), P(("inner", "wide"), None))
    return jax.shard_map(
        on_device, mesh=mesh, in_specs=in_specs, out_specs=out_specs, check_vma=False
    )
```

```python
import jax
import jax.numpy as jnp
from jax import lax
from jax.experimental import pallas as pl
from jax.experimental.pallas import tpu as pltpu
from jax.sharding import PartitionSpec as P


BLOCK = 128
SLAB = 8


def hdot(left, right):
    return jnp.dot(left, right, precision=lax.Precision.HIGHEST, preferred_element_type=jnp.float32)


def sweep_block(diag):
    size = diag.shape[0]
    eye = (lax.broadcasted_iota(jnp.int32, (size, size), 0) == lax.broadcasted_iota(jnp.int32, (size, size), 1)).astype(jnp.float32)
    joined = jnp.concatenate([diag, eye], axis=1)
    slabs = [joined[s * SLAB:(s + 1) * SLAB] for s in range(size // SLAB)]
    rows = lax.broadcasted_iota(jnp.int32, (SLAB, 1), 0)
    for j in range(size):
        s, t = divmod(j, SLAB)
        scale = lax.rsqrt(slabs[s][t:t + 1, j:j + 1])
        top = slabs[s][t:t + 1, :] * scale
        for q in range(s + 1, len(slabs)):
            slabs[q] = slabs[q] - (slabs[q][:, j:j + 1] * scale) * top
        here = slabs[s]
        updated = here - (here[:, j:j + 1] * scale) * top
        slabs[s] = jnp.where(rows > t, updated, jnp.where(rows == t, top, here))
    joined = jnp.concatenate(slabs, axis=0)
    r = lax.broadcasted_iota(jnp.int32, (size, size), 0)
    c = lax.broadcasted_iota(jnp.int32, (size, size), 1)
    return jnp.where(c >= r, joined[:, :size], 0.0), joined[:, size:]


def chol_kernel(g_ref, u_ref, inv_ref, work_ref, aug_ref):
    n = g_ref.shape[0]
    g = g_ref[...]
    work_ref[...] = (g + g.T) * 0.5
    aug_ref[...] = jnp.zeros_like(aug_ref)
    u_ref[...] = jnp.zeros_like(u_ref)
    inv_ref[...] = jnp.zeros_like(inv_ref)
    blocks = n // BLOCK
    for k in range(blocks):
        lo, hi = k * BLOCK, (k + 1) * BLOCK
        u_kk, inv_kk = sweep_block(work_ref[lo:hi, lo:hi])
        u_ref[lo:hi, lo:hi] = u_kk
        if k > 0:
            inv_ref[lo:hi, 0:lo] = hdot(inv_kk, aug_ref[lo:hi, 0:lo])
        inv_ref[lo:hi, lo:hi] = inv_kk
        if hi < n:
            u_off = hdot(inv_kk, work_ref[lo:hi, hi:n])
            u_ref[lo:hi, hi:n] = u_off
            u_off_t = u_off.T
            work_ref[hi:n, hi:n] = work_ref[hi:n, hi:n] - hdot(u_off_t, u_off)
            aug_ref[hi:n, 0:hi] = aug_ref[hi:n, 0:hi] - hdot(u_off_t, inv_ref[lo:hi, 0:hi])


def cholesky_and_inverse(gram_matrix):
    n = gram_matrix.shape[0]
    spec = pl.BlockSpec(memory_space=pltpu.VMEM)
    return pl.pallas_call(
        chol_kernel,
        out_shape=(jax.ShapeDtypeStruct((n, n), jnp.float32), jax.ShapeDtypeStruct((n, n), jnp.float32)),
        in_specs=[spec],
        out_specs=(spec, spec),
        scratch_shapes=[pltpu.VMEM((n, n), jnp.float32), pltpu.VMEM((n, n), jnp.float32)],
    )(gram_matrix)


def matmul(left, right):
    return jnp.dot(left, right, precision=lax.Precision.HIGHEST, preferred_element_type=jnp.float32)


def gram_of(matrix):
    return lax.dot_general(
        matrix,
        matrix,
        (((0,), (0,)), ((), ())),
        precision=lax.Precision.HIGHEST,
        preferred_element_type=jnp.float32,
    )


def group_index(axis, shift, size):
    return (lax.axis_index(axis) >> shift) & (size - 1)


def partner_xor(value, axis, shift, offset):
    mask = offset << shift
    pairs = [(source, source ^ mask) for source in range(lax.axis_size(axis))]
    return lax.ppermute(value, axis, pairs)


def scatter_sum(value, axis, shift, size):
    height = value.shape[0] // size
    index = group_index(axis, shift, size)
    chunk = lambda j: lax.dynamic_slice_in_dim(value, j * height, height, 0)
    total = chunk(index)
    for offset in range(1, size):
        total = total + partner_xor(chunk(index ^ offset), axis, shift, offset)
    return total


def gather_all(chunk, axis, shift, size):
    height = chunk.shape[0]
    index = group_index(axis, shift, size)
    whole = jnp.zeros((height * size, chunk.shape[1]), chunk.dtype)
    whole = lax.dynamic_update_slice_in_dim(whole, chunk, index * height, 0)
    for offset in range(1, size):
        got = partner_xor(chunk, axis, shift, offset)
        whole = lax.dynamic_update_slice_in_dim(whole, got, (index ^ offset) * height, 0)
    return whole


def axis_groups(axis, first):
    bits = lax.axis_size(axis).bit_length() - 1
    groups = []
    shift = first
    while shift < bits:
        width = min(2, bits - shift)
        groups.append((axis, shift, 2**width))
        shift += width
    return groups


def all_sum(gram_matrix):
    groups = [("wide", 0, 2)] + axis_groups("inner", 0) + axis_groups("wide", 1)
    for group in groups:
        gram_matrix = scatter_sum(gram_matrix, *group)
    for group in reversed(groups):
        gram_matrix = gather_all(gram_matrix, *group)
    return gram_matrix


def on_device(response):
    row_count = response.shape[0] * lax.axis_size("inner") * lax.axis_size("wide")
    gram_matrix = gram_of(response) / row_count
    gram_matrix = all_sum(gram_matrix)
    upper_factor, inverse_lower = cholesky_and_inverse(gram_matrix)
    q_rows = lax.dot_general(
        response,
        inverse_lower,
        (((1,), (1,)), ((), ())),
        precision=lax.Precision.HIGHEST,
        preferred_element_type=jnp.float32,
    )
    return (upper_factor, q_rows)


def solution(mesh):
    in_specs = (P(("inner", "wide"), None),)
    out_specs = (P(), P(("inner", "wide"), None))
    return jax.shard_map(
        on_device, mesh=mesh, in_specs=in_specs, out_specs=out_specs, check_vma=False
    )
```

```python
import jax
import jax.numpy as jnp
from jax import lax
from jax.experimental import pallas as pl
from jax.experimental.pallas import tpu as pltpu
from jax.sharding import PartitionSpec as P


BLOCK = 128
SLAB = 8


def hdot(left, right):
    return jnp.dot(left, right, precision=lax.Precision.HIGHEST, preferred_element_type=jnp.float32)


def sweep_block(diag):
    size = diag.shape[0]
    eye = (lax.broadcasted_iota(jnp.int32, (size, size), 0) == lax.broadcasted_iota(jnp.int32, (size, size), 1)).astype(jnp.float32)
    joined = jnp.concatenate([diag, eye], axis=1)
    slabs = [joined[s * SLAB:(s + 1) * SLAB] for s in range(size // SLAB)]
    rows = lax.broadcasted_iota(jnp.int32, (SLAB, 1), 0)
    for j in range(size):
        s, t = divmod(j, SLAB)
        scale = lax.rsqrt(slabs[s][t:t + 1, j:j + 1])
        top = slabs[s][t:t + 1, :] * scale
        for q in range(s + 1, len(slabs)):
            slabs[q] = slabs[q] - (slabs[q][:, j:j + 1] * scale) * top
        here = slabs[s]
        updated = here - (here[:, j:j + 1] * scale) * top
        slabs[s] = jnp.where(rows > t, updated, jnp.where(rows == t, top, here))
    joined = jnp.concatenate(slabs, axis=0)
    r = lax.broadcasted_iota(jnp.int32, (size, size), 0)
    c = lax.broadcasted_iota(jnp.int32, (size, size), 1)
    return jnp.where(c >= r, joined[:, :size], 0.0), joined[:, size:]


def chol_kernel(g_ref, u_ref, uinv_ref, work_ref, aug_ref, inv_ref):
    n = g_ref.shape[0]
    g = g_ref[...]
    work_ref[...] = (g + g.T) * 0.5
    aug_ref[...] = jnp.zeros_like(aug_ref)
    u_ref[...] = jnp.zeros_like(u_ref)
    uinv_ref[...] = jnp.zeros_like(uinv_ref)
    inv_ref[...] = jnp.zeros_like(inv_ref)
    blocks = n // BLOCK
    for k in range(blocks):
        lo, hi = k * BLOCK, (k + 1) * BLOCK
        u_kk, inv_kk = sweep_block(work_ref[lo:hi, lo:hi])
        u_ref[lo:hi, lo:hi] = u_kk
        if k > 0:
            inv_row = hdot(inv_kk, aug_ref[lo:hi, 0:lo])
            inv_ref[lo:hi, 0:lo] = inv_row
            uinv_ref[0:lo, lo:hi] = inv_row.T
        inv_ref[lo:hi, lo:hi] = inv_kk
        uinv_ref[lo:hi, lo:hi] = inv_kk.T
        if hi < n:
            u_off = hdot(inv_kk, work_ref[lo:hi, hi:n])
            u_ref[lo:hi, hi:n] = u_off
            u_off_t = u_off.T
            work_ref[hi:n, hi:n] = work_ref[hi:n, hi:n] - hdot(u_off_t, u_off)
            aug_ref[hi:n, 0:hi] = aug_ref[hi:n, 0:hi] - hdot(u_off_t, inv_ref[lo:hi, 0:hi])


def cholesky_and_inverse(gram_matrix):
    n = gram_matrix.shape[0]
    spec = pl.BlockSpec(memory_space=pltpu.VMEM)
    return pl.pallas_call(
        chol_kernel,
        out_shape=(jax.ShapeDtypeStruct((n, n), jnp.float32), jax.ShapeDtypeStruct((n, n), jnp.float32)),
        in_specs=[spec],
        out_specs=(spec, spec),
        scratch_shapes=[pltpu.VMEM((n, n), jnp.float32) for _ in range(3)],
    )(gram_matrix)


def rows_kernel(a_ref, w_ref, o_ref):
    o_ref[...] = hdot(a_ref[...], w_ref[...])


def rows_times(matrix, weights):
    rows, width = matrix.shape
    tile = min(rows, 512)
    return pl.pallas_call(
        rows_kernel,
        out_shape=jax.ShapeDtypeStruct((rows, weights.shape[1]), jnp.float32),
        grid=(rows // tile,),
        in_specs=[
            pl.BlockSpec((tile, width), lambda i: (i, 0)),
            pl.BlockSpec(weights.shape, lambda i: (0, 0)),
        ],
        out_specs=pl.BlockSpec((tile, weights.shape[1]), lambda i: (i, 0)),
    )(matrix, weights)


def matmul(left, right):
    return jnp.dot(left, right, precision=lax.Precision.HIGHEST, preferred_element_type=jnp.float32)


def gram_of(matrix):
    return lax.dot_general(
        matrix,
        matrix,
        (((0,), (0,)), ((), ())),
        precision=lax.Precision.HIGHEST,
        preferred_element_type=jnp.float32,
    )


def group_index(axis, shift, size):
    return (lax.axis_index(axis) >> shift) & (size - 1)


def partner_xor(value, axis, shift, offset):
    mask = offset << shift
    pairs = [(source, source ^ mask) for source in range(lax.axis_size(axis))]
    return lax.ppermute(value, axis, pairs)


def scatter_sum(value, axis, shift, size):
    height = value.shape[0] // size
    index = group_index(axis, shift, size)
    chunk = lambda j: lax.dynamic_slice_in_dim(value, j * height, height, 0)
    total = chunk(index)
    for offset in range(1, size):
        total = total + partner_xor(chunk(index ^ offset), axis, shift, offset)
    return total


def gather_all(chunk, axis, shift, size):
    height = chunk.shape[0]
    index = group_index(axis, shift, size)
    whole = jnp.zeros((height * size, chunk.shape[1]), chunk.dtype)
    whole = lax.dynamic_update_slice_in_dim(whole, chunk, index * height, 0)
    for offset in range(1, size):
        got = partner_xor(chunk, axis, shift, offset)
        whole = lax.dynamic_update_slice_in_dim(whole, got, (index ^ offset) * height, 0)
    return whole


def axis_groups(axis, first):
    bits = lax.axis_size(axis).bit_length() - 1
    groups = []
    shift = first
    while shift < bits:
        width = min(2, bits - shift)
        groups.append((axis, shift, 2**width))
        shift += width
    return groups


def all_sum(gram_matrix):
    groups = [("wide", 0, 2)] + axis_groups("inner", 0) + axis_groups("wide", 1)
    for group in groups:
        gram_matrix = scatter_sum(gram_matrix, *group)
    for group in reversed(groups):
        gram_matrix = gather_all(gram_matrix, *group)
    return gram_matrix


def on_device(response):
    row_count = response.shape[0] * lax.axis_size("inner") * lax.axis_size("wide")
    gram_matrix = gram_of(response) / row_count
    gram_matrix = all_sum(gram_matrix)
    upper_factor, inverse_upper = cholesky_and_inverse(gram_matrix)
    q_rows = rows_times(response, inverse_upper)
    return (upper_factor, q_rows)


def solution(mesh):
    in_specs = (P(("inner", "wide"), None),)
    out_specs = (P(), P(("inner", "wide"), None))
    return jax.shard_map(
        on_device, mesh=mesh, in_specs=in_specs, out_specs=out_specs, check_vma=False
    )
```

```python
import jax
import jax.numpy as jnp
from jax import lax
from jax.experimental import pallas as pl
from jax.experimental.pallas import tpu as pltpu
from jax.sharding import PartitionSpec as P


BLOCK = 128
SLAB = 8


def hdot(left, right):
    return jnp.dot(left, right, precision=lax.Precision.HIGHEST, preferred_element_type=jnp.float32)


def sweep_block(diag):
    size = diag.shape[0]
    eye = (lax.broadcasted_iota(jnp.int32, (size, size), 0) == lax.broadcasted_iota(jnp.int32, (size, size), 1)).astype(jnp.float32)
    joined = jnp.concatenate([diag, eye], axis=1)
    slabs = [joined[s * SLAB:(s + 1) * SLAB] for s in range(size // SLAB)]
    rows = lax.broadcasted_iota(jnp.int32, (SLAB, 1), 0)
    for j in range(size):
        s, t = divmod(j, SLAB)
        scale = lax.rsqrt(slabs[s][t:t + 1, j:j + 1])
        top = slabs[s][t:t + 1, :] * scale
        for q in range(s + 1, len(slabs)):
            slabs[q] = slabs[q] - (slabs[q][:, j:j + 1] * scale) * top
        here = slabs[s]
        updated = here - (here[:, j:j + 1] * scale) * top
        slabs[s] = jnp.where(rows > t, updated, jnp.where(rows == t, top, here))
    joined = jnp.concatenate(slabs, axis=0)
    r = lax.broadcasted_iota(jnp.int32, (size, size), 0)
    c = lax.broadcasted_iota(jnp.int32, (size, size), 1)
    return jnp.where(c >= r, joined[:, :size], 0.0), joined[:, size:]


def chol_kernel(g_ref, u_ref, uinv_ref, work_ref, aug_ref, inv_ref):
    n = g_ref.shape[0]
    g = g_ref[...]
    work_ref[...] = (g + g.T) * 0.5
    aug_ref[...] = jnp.zeros_like(aug_ref)
    u_ref[...] = jnp.zeros_like(u_ref)
    uinv_ref[...] = jnp.zeros_like(uinv_ref)
    inv_ref[...] = jnp.zeros_like(inv_ref)
    blocks = n // BLOCK
    for k in range(blocks):
        lo, hi = k * BLOCK, (k + 1) * BLOCK
        u_kk, inv_kk = sweep_block(work_ref[lo:hi, lo:hi])
        u_ref[lo:hi, lo:hi] = u_kk
        if k > 0:
            inv_row = hdot(inv_kk, aug_ref[lo:hi, 0:lo])
            inv_ref[lo:hi, 0:lo] = inv_row
            uinv_ref[0:lo, lo:hi] = inv_row.T
        inv_ref[lo:hi, lo:hi] = inv_kk
        uinv_ref[lo:hi, lo:hi] = inv_kk.T
        if hi < n:
            u_off = hdot(inv_kk, work_ref[lo:hi, hi:n])
            u_ref[lo:hi, hi:n] = u_off
            u_off_t = u_off.T
            work_ref[hi:n, hi:n] = work_ref[hi:n, hi:n] - hdot(u_off_t, u_off)
            aug_ref[hi:n, 0:hi] = aug_ref[hi:n, 0:hi] - hdot(u_off_t, inv_ref[lo:hi, 0:hi])


def cholesky_and_inverse(gram_matrix):
    n = gram_matrix.shape[0]
    spec = pl.BlockSpec(memory_space=pltpu.VMEM)
    return pl.pallas_call(
        chol_kernel,
        out_shape=(jax.ShapeDtypeStruct((n, n), jnp.float32), jax.ShapeDtypeStruct((n, n), jnp.float32)),
        in_specs=[spec],
        out_specs=(spec, spec),
        scratch_shapes=[pltpu.VMEM((n, n), jnp.float32) for _ in range(3)],
    )(gram_matrix)


def rows_kernel(a_ref, w_ref, o_ref):
    width = w_ref.shape[1]
    half = width // 2
    o_ref[:, 0:half] = hdot(a_ref[:, 0:half], w_ref[0:half, 0:half])
    o_ref[:, half:width] = hdot(a_ref[...], w_ref[:, half:width])


def rows_times(matrix, weights):
    rows, width = matrix.shape
    tile = min(rows, 512)
    return pl.pallas_call(
        rows_kernel,
        out_shape=jax.ShapeDtypeStruct((rows, weights.shape[1]), jnp.float32),
        grid=(rows // tile,),
        in_specs=[
            pl.BlockSpec((tile, width), lambda i: (i, 0)),
            pl.BlockSpec(weights.shape, lambda i: (0, 0)),
        ],
        out_specs=pl.BlockSpec((tile, weights.shape[1]), lambda i: (i, 0)),
    )(matrix, weights)


def matmul(left, right):
    return jnp.dot(left, right, precision=lax.Precision.HIGHEST, preferred_element_type=jnp.float32)


def cross(left, right):
    return lax.dot_general(
        left,
        right,
        (((0,), (0,)), ((), ())),
        precision=lax.Precision.HIGHEST,
        preferred_element_type=jnp.float32,
    )


def gram_of(matrix):
    half = matrix.shape[1] // 2
    first = cross(matrix, matrix[:, :half])
    corner = cross(matrix[:, half:], matrix[:, half:])
    second = jnp.concatenate([first[half:].T, corner], axis=0)
    return jnp.concatenate([first, second], axis=1)


def group_index(axis, shift, size):
    return (lax.axis_index(axis) >> shift) & (size - 1)


def partner_xor(value, axis, shift, offset):
    mask = offset << shift
    pairs = [(source, source ^ mask) for source in range(lax.axis_size(axis))]
    return lax.ppermute(value, axis, pairs)


def scatter_sum(value, axis, shift, size):
    height = value.shape[0] // size
    index = group_index(axis, shift, size)
    chunk = lambda j: lax.dynamic_slice_in_dim(value, j * height, height, 0)
    total = chunk(index)
    for offset in range(1, size):
        total = total + partner_xor(chunk(index ^ offset), axis, shift, offset)
    return total


def gather_all(chunk, axis, shift, size):
    height = chunk.shape[0]
    index = group_index(axis, shift, size)
    whole = jnp.zeros((height * size, chunk.shape[1]), chunk.dtype)
    whole = lax.dynamic_update_slice_in_dim(whole, chunk, index * height, 0)
    for offset in range(1, size):
        got = partner_xor(chunk, axis, shift, offset)
        whole = lax.dynamic_update_slice_in_dim(whole, got, (index ^ offset) * height, 0)
    return whole


def axis_groups(axis, first):
    bits = lax.axis_size(axis).bit_length() - 1
    groups = []
    shift = first
    while shift < bits:
        width = min(2, bits - shift)
        groups.append((axis, shift, 2**width))
        shift += width
    return groups


def all_sum(gram_matrix):
    groups = [("wide", 0, 2)] + axis_groups("inner", 0) + axis_groups("wide", 1)
    for group in groups:
        gram_matrix = scatter_sum(gram_matrix, *group)
    for group in reversed(groups):
        gram_matrix = gather_all(gram_matrix, *group)
    return gram_matrix


def on_device(response):
    row_count = response.shape[0] * lax.axis_size("inner") * lax.axis_size("wide")
    gram_matrix = gram_of(response) / row_count
    gram_matrix = all_sum(gram_matrix)
    upper_factor, inverse_upper = cholesky_and_inverse(gram_matrix)
    q_rows = rows_times(response, inverse_upper)
    return (upper_factor, q_rows)


def solution(mesh):
    in_specs = (P(("inner", "wide"), None),)
    out_specs = (P(), P(("inner", "wide"), None))
    return jax.shard_map(
        on_device, mesh=mesh, in_specs=in_specs, out_specs=out_specs, check_vma=False
    )
```

```python
import jax
import jax.numpy as jnp
from jax import lax
from jax.experimental import pallas as pl
from jax.experimental.pallas import tpu as pltpu
from jax.sharding import PartitionSpec as P


BLOCK = 128
SLAB = 8


def hdot(left, right):
    return jnp.dot(left, right, precision=lax.Precision.HIGHEST, preferred_element_type=jnp.float32)


def sweep_block(diag):
    size = diag.shape[0]
    eye = (lax.broadcasted_iota(jnp.int32, (size, size), 0) == lax.broadcasted_iota(jnp.int32, (size, size), 1)).astype(jnp.float32)
    joined = jnp.concatenate([diag, eye], axis=1)
    slabs = [joined[s * SLAB:(s + 1) * SLAB] for s in range(size // SLAB)]
    rows = lax.broadcasted_iota(jnp.int32, (SLAB, 1), 0)
    for j in range(size):
        s, t = divmod(j, SLAB)
        scale = lax.rsqrt(slabs[s][t:t + 1, j:j + 1])
        top = slabs[s][t:t + 1, :] * scale
        for q in range(s + 1, len(slabs)):
            slabs[q] = slabs[q] - (slabs[q][:, j:j + 1] * scale) * top
        here = slabs[s]
        updated = here - (here[:, j:j + 1] * scale) * top
        slabs[s] = jnp.where(rows > t, updated, jnp.where(rows == t, top, here))
    joined = jnp.concatenate(slabs, axis=0)
    r = lax.broadcasted_iota(jnp.int32, (size, size), 0)
    c = lax.broadcasted_iota(jnp.int32, (size, size), 1)
    return jnp.where(c >= r, joined[:, :size], 0.0), joined[:, size:]


def chol_kernel(g_ref, u_ref, uinv_ref, work_ref, aug_ref, inv_ref):
    n = g_ref.shape[0]
    g = g_ref[...]
    work_ref[...] = (g + g.T) * 0.5
    aug_ref[...] = jnp.zeros_like(aug_ref)
    u_ref[...] = jnp.zeros_like(u_ref)
    uinv_ref[...] = jnp.zeros_like(uinv_ref)
    inv_ref[...] = jnp.zeros_like(inv_ref)
    blocks = n // BLOCK
    for k in range(blocks):
        lo, hi = k * BLOCK, (k + 1) * BLOCK
        u_kk, inv_kk = sweep_block(work_ref[lo:hi, lo:hi])
        u_ref[lo:hi, lo:hi] = u_kk
        if k > 0:
            inv_row = hdot(inv_kk, aug_ref[lo:hi, 0:lo])
            inv_ref[lo:hi, 0:lo] = inv_row
            uinv_ref[0:lo, lo:hi] = inv_row.T
        inv_ref[lo:hi, lo:hi] = inv_kk
        uinv_ref[lo:hi, lo:hi] = inv_kk.T
        if hi < n:
            u_off = hdot(inv_kk, work_ref[lo:hi, hi:n])
            u_ref[lo:hi, hi:n] = u_off
            u_off_t = u_off.T
            work_ref[hi:n, hi:n] = work_ref[hi:n, hi:n] - hdot(u_off_t, u_off)
            aug_ref[hi:n, 0:hi] = aug_ref[hi:n, 0:hi] - hdot(u_off_t, inv_ref[lo:hi, 0:hi])


def cholesky_and_inverse(gram_matrix):
    n = gram_matrix.shape[0]
    spec = pl.BlockSpec(memory_space=pltpu.VMEM)
    return pl.pallas_call(
        chol_kernel,
        out_shape=(jax.ShapeDtypeStruct((n, n), jnp.float32), jax.ShapeDtypeStruct((n, n), jnp.float32)),
        in_specs=[spec],
        out_specs=(spec, spec),
        scratch_shapes=[pltpu.VMEM((n, n), jnp.float32) for _ in range(3)],
    )(gram_matrix)


def rows_kernel(a_ref, w_ref, o_ref):
    width = w_ref.shape[1]
    half = width // 2
    o_ref[:, 0:half] = hdot(a_ref[:, 0:half], w_ref[0:half, 0:half])
    o_ref[:, half:width] = hdot(a_ref[...], w_ref[:, half:width])


def rows_times(matrix, weights):
    rows, width = matrix.shape
    tile = min(rows, 512)
    return pl.pallas_call(
        rows_kernel,
        out_shape=jax.ShapeDtypeStruct((rows, weights.shape[1]), jnp.float32),
        grid=(rows // tile,),
        in_specs=[
            pl.BlockSpec((tile, width), lambda i: (i, 0)),
            pl.BlockSpec(weights.shape, lambda i: (0, 0)),
        ],
        out_specs=pl.BlockSpec((tile, weights.shape[1]), lambda i: (i, 0)),
    )(matrix, weights)


def matmul(left, right):
    return jnp.dot(left, right, precision=lax.Precision.HIGHEST, preferred_element_type=jnp.float32)


def gram_of(matrix):
    return lax.dot_general(
        matrix,
        matrix,
        (((0,), (0,)), ((), ())),
        precision=lax.Precision.HIGHEST,
        preferred_element_type=jnp.float32,
    )


def group_index(axis, shift, size):
    return (lax.axis_index(axis) >> shift) & (size - 1)


def partner_xor(value, axis, shift, offset):
    mask = offset << shift
    pairs = [(source, source ^ mask) for source in range(lax.axis_size(axis))]
    return lax.ppermute(value, axis, pairs)


def scatter_sum(value, axis, shift, size):
    height = value.shape[0] // size
    index = group_index(axis, shift, size)
    chunk = lambda j: lax.dynamic_slice_in_dim(value, j * height, height, 0)
    total = chunk(index)
    for offset in range(1, size):
        total = total + partner_xor(chunk(index ^ offset), axis, shift, offset)
    return total


def gather_all(chunk, axis, shift, size):
    height = chunk.shape[0]
    index = group_index(axis, shift, size)
    whole = jnp.zeros((height * size, chunk.shape[1]), chunk.dtype)
    whole = lax.dynamic_update_slice_in_dim(whole, chunk, index * height, 0)
    for offset in range(1, size):
        got = partner_xor(chunk, axis, shift, offset)
        whole = lax.dynamic_update_slice_in_dim(whole, got, (index ^ offset) * height, 0)
    return whole


def axis_groups(axis, first):
    bits = lax.axis_size(axis).bit_length() - 1
    groups = []
    shift = first
    while shift < bits:
        width = min(2, bits - shift)
        groups.append((axis, shift, 2**width))
        shift += width
    return groups


def all_sum(gram_matrix):
    groups = [("wide", 0, 2)] + axis_groups("inner", 0) + axis_groups("wide", 1)
    for group in groups:
        gram_matrix = scatter_sum(gram_matrix, *group)
    for group in reversed(groups):
        gram_matrix = gather_all(gram_matrix, *group)
    return gram_matrix


def on_device(response):
    row_count = response.shape[0] * lax.axis_size("inner") * lax.axis_size("wide")
    gram_matrix = gram_of(response) / row_count
    gram_matrix = all_sum(gram_matrix)
    upper_factor, inverse_upper = cholesky_and_inverse(gram_matrix)
    q_rows = rows_times(response, inverse_upper)
    return (upper_factor, q_rows)


def solution(mesh):
    in_specs = (P(("inner", "wide"), None),)
    out_specs = (P(), P(("inner", "wide"), None))
    return jax.shard_map(
        on_device, mesh=mesh, in_specs=in_specs, out_specs=out_specs, check_vma=False
    )
```

```python
import functools

import jax
import jax.numpy as jnp
from jax import lax
from jax.experimental import pallas as pl
from jax.experimental.pallas import tpu as pltpu
from jax.sharding import PartitionSpec as P


BLOCK = 128
SLAB = 8


def hdot(left, right):
    return jnp.dot(left, right, precision=lax.Precision.HIGHEST, preferred_element_type=jnp.float32)


def sweep_block(diag):
    size = diag.shape[0]
    eye = (lax.broadcasted_iota(jnp.int32, (size, size), 0) == lax.broadcasted_iota(jnp.int32, (size, size), 1)).astype(jnp.float32)
    joined = jnp.concatenate([diag, eye], axis=1)
    slabs = [joined[s * SLAB:(s + 1) * SLAB] for s in range(size // SLAB)]
    rows = lax.broadcasted_iota(jnp.int32, (SLAB, 1), 0)
    for j in range(size):
        s, t = divmod(j, SLAB)
        scale = lax.rsqrt(slabs[s][t:t + 1, j:j + 1])
        top = slabs[s][t:t + 1, :] * scale
        for q in range(s + 1, len(slabs)):
            slabs[q] = slabs[q] - (slabs[q][:, j:j + 1] * scale) * top
        here = slabs[s]
        updated = here - (here[:, j:j + 1] * scale) * top
        slabs[s] = jnp.where(rows > t, updated, jnp.where(rows == t, top, here))
    joined = jnp.concatenate(slabs, axis=0)
    r = lax.broadcasted_iota(jnp.int32, (size, size), 0)
    c = lax.broadcasted_iota(jnp.int32, (size, size), 1)
    return jnp.where(c >= r, joined[:, :size], 0.0), joined[:, size:]


def chol_kernel(g_ref, u_ref, uinv_ref, work_ref, aug_ref, inv_ref):
    n = g_ref.shape[0]
    g = g_ref[...]
    work_ref[...] = (g + g.T) * 0.5
    aug_ref[...] = jnp.zeros_like(aug_ref)
    u_ref[...] = jnp.zeros_like(u_ref)
    uinv_ref[...] = jnp.zeros_like(uinv_ref)
    inv_ref[...] = jnp.zeros_like(inv_ref)
    blocks = n // BLOCK
    for k in range(blocks):
        lo, hi = k * BLOCK, (k + 1) * BLOCK
        u_kk, inv_kk = sweep_block(work_ref[lo:hi, lo:hi])
        u_ref[lo:hi, lo:hi] = u_kk
        if k > 0:
            inv_row = hdot(inv_kk, aug_ref[lo:hi, 0:lo])
            inv_ref[lo:hi, 0:lo] = inv_row
            uinv_ref[0:lo, lo:hi] = inv_row.T
        inv_ref[lo:hi, lo:hi] = inv_kk
        uinv_ref[lo:hi, lo:hi] = inv_kk.T
        if hi < n:
            u_off = hdot(inv_kk, work_ref[lo:hi, hi:n])
            u_ref[lo:hi, hi:n] = u_off
            u_off_t = u_off.T
            work_ref[hi:n, hi:n] = work_ref[hi:n, hi:n] - hdot(u_off_t, u_off)
            aug_ref[hi:n, 0:hi] = aug_ref[hi:n, 0:hi] - hdot(u_off_t, inv_ref[lo:hi, 0:hi])


def cholesky_and_inverse(gram_matrix):
    n = gram_matrix.shape[0]
    spec = pl.BlockSpec(memory_space=pltpu.VMEM)
    return pl.pallas_call(
        chol_kernel,
        out_shape=(jax.ShapeDtypeStruct((n, n), jnp.float32), jax.ShapeDtypeStruct((n, n), jnp.float32)),
        in_specs=[spec],
        out_specs=(spec, spec),
        scratch_shapes=[pltpu.VMEM((n, n), jnp.float32) for _ in range(3)],
    )(gram_matrix)


def rows_kernel(a_ref, w_ref, o_ref):
    width = w_ref.shape[1]
    half = width // 2
    o_ref[:, 0:half] = hdot(a_ref[:, 0:half], w_ref[0:half, 0:half])
    o_ref[:, half:width] = hdot(a_ref[...], w_ref[:, half:width])


def rows_times(matrix, weights):
    rows, width = matrix.shape
    tile = min(rows, 512)
    return pl.pallas_call(
        rows_kernel,
        out_shape=jax.ShapeDtypeStruct((rows, weights.shape[1]), jnp.float32),
        grid=(rows // tile,),
        in_specs=[
            pl.BlockSpec((tile, width), lambda i: (i, 0)),
            pl.BlockSpec(weights.shape, lambda i: (0, 0)),
        ],
        out_specs=pl.BlockSpec((tile, weights.shape[1]), lambda i: (i, 0)),
    )(matrix, weights)


def matmul(left, right):
    return jnp.dot(left, right, precision=lax.Precision.HIGHEST, preferred_element_type=jnp.float32)


def cross(left, right):
    return lax.dot_general(
        left,
        right,
        (((0,), (0,)), ((), ())),
        precision=lax.Precision.HIGHEST,
        preferred_element_type=jnp.float32,
    )


def gram_kernel(row_count, a_ref, o_ref):
    step = pl.program_id(0)
    half = a_ref.shape[1] // 2

    @pl.when(step == 0)
    def _():
        o_ref[...] = jnp.zeros_like(o_ref)

    a = a_ref[...]
    o_ref[:, 0:half] += cross(a, a[:, 0:half])
    o_ref[half:, half:] += cross(a[:, half:], a[:, half:])

    @pl.when(step == pl.num_programs(0) - 1)
    def _():
        o_ref[0:half, half:] = o_ref[half:, 0:half].T
        o_ref[...] = o_ref[...] / row_count


def gram_of(matrix, row_count):
    rows, width = matrix.shape
    tile = min(rows, 512)
    return pl.pallas_call(
        functools.partial(gram_kernel, row_count),
        out_shape=jax.ShapeDtypeStruct((width, width), jnp.float32),
        grid=(rows // tile,),
        in_specs=[pl.BlockSpec((tile, width), lambda i: (i, 0))],
        out_specs=pl.BlockSpec((width, width), lambda i: (0, 0)),
    )(matrix)


def group_index(axis, shift, size):
    return (lax.axis_index(axis) >> shift) & (size - 1)


def partner_xor(value, axis, shift, offset):
    mask = offset << shift
    pairs = [(source, source ^ mask) for source in range(lax.axis_size(axis))]
    return lax.ppermute(value, axis, pairs)


def scatter_sum(value, axis, shift, size):
    height = value.shape[0] // size
    index = group_index(axis, shift, size)
    chunk = lambda j: lax.dynamic_slice_in_dim(value, j * height, height, 0)
    total = chunk(index)
    for offset in range(1, size):
        total = total + partner_xor(chunk(index ^ offset), axis, shift, offset)
    return total


def gather_all(chunk, axis, shift, size):
    height = chunk.shape[0]
    index = group_index(axis, shift, size)
    whole = jnp.zeros((height * size, chunk.shape[1]), chunk.dtype)
    whole = lax.dynamic_update_slice_in_dim(whole, chunk, index * height, 0)
    for offset in range(1, size):
        got = partner_xor(chunk, axis, shift, offset)
        whole = lax.dynamic_update_slice_in_dim(whole, got, (index ^ offset) * height, 0)
    return whole


def axis_groups(axis, first):
    bits = lax.axis_size(axis).bit_length() - 1
    groups = []
    shift = first
    while shift < bits:
        width = min(2, bits - shift)
        groups.append((axis, shift, 2**width))
        shift += width
    return groups


def all_sum(gram_matrix):
    groups = [("wide", 0, 2)] + axis_groups("inner", 0) + axis_groups("wide", 1)
    for group in groups:
        gram_matrix = scatter_sum(gram_matrix, *group)
    for group in reversed(groups):
        gram_matrix = gather_all(gram_matrix, *group)
    return gram_matrix


def on_device(response):
    row_count = response.shape[0] * lax.axis_size("inner") * lax.axis_size("wide")
    gram_matrix = gram_of(response, row_count)
    gram_matrix = all_sum(gram_matrix)
    upper_factor, inverse_upper = cholesky_and_inverse(gram_matrix)
    q_rows = rows_times(response, inverse_upper)
    return (upper_factor, q_rows)


def solution(mesh):
    in_specs = (P(("inner", "wide"), None),)
    out_specs = (P(), P(("inner", "wide"), None))
    return jax.shard_map(
        on_device, mesh=mesh, in_specs=in_specs, out_specs=out_specs, check_vma=False
    )
```

```python
import functools

import jax
import jax.numpy as jnp
from jax import lax
from jax.experimental import pallas as pl
from jax.experimental.pallas import tpu as pltpu
from jax.sharding import PartitionSpec as P


BLOCK = 128
SLAB = 8


def hdot(left, right):
    return jnp.dot(left, right, precision=lax.Precision.HIGHEST, preferred_element_type=jnp.float32)


def sweep_block(diag):
    size = diag.shape[0]
    eye = (lax.broadcasted_iota(jnp.int32, (size, size), 0) == lax.broadcasted_iota(jnp.int32, (size, size), 1)).astype(jnp.float32)
    joined = jnp.concatenate([diag, eye], axis=1)
    slabs = [joined[s * SLAB:(s + 1) * SLAB] for s in range(size // SLAB)]
    rows = lax.broadcasted_iota(jnp.int32, (SLAB, 1), 0)
    for j in range(size):
        s, t = divmod(j, SLAB)
        scale = lax.rsqrt(slabs[s][t:t + 1, j:j + 1])
        top = slabs[s][t:t + 1, :] * scale
        for q in range(s + 1, len(slabs)):
            slabs[q] = slabs[q] - (slabs[q][:, j:j + 1] * scale) * top
        here = slabs[s]
        updated = here - (here[:, j:j + 1] * scale) * top
        slabs[s] = jnp.where(rows > t, updated, jnp.where(rows == t, top, here))
    joined = jnp.concatenate(slabs, axis=0)
    r = lax.broadcasted_iota(jnp.int32, (size, size), 0)
    c = lax.broadcasted_iota(jnp.int32, (size, size), 1)
    return jnp.where(c >= r, joined[:, :size], 0.0), joined[:, size:]


def chol_kernel(bit_ref, mine_ref, got_ref, u_ref, uinv_ref, work_ref, aug_ref, inv_ref):
    n = u_ref.shape[0]
    half = n // 2

    @pl.when(bit_ref[0] == 0)
    def _():
        work_ref[0:half, :] = mine_ref[...]
        work_ref[half:n, :] = got_ref[...]

    @pl.when(bit_ref[0] != 0)
    def _():
        work_ref[0:half, :] = got_ref[...]
        work_ref[half:n, :] = mine_ref[...]

    g = work_ref[...]
    work_ref[...] = (g + g.T) * 0.5
    aug_ref[...] = jnp.zeros_like(aug_ref)
    u_ref[...] = jnp.zeros_like(u_ref)
    uinv_ref[...] = jnp.zeros_like(uinv_ref)
    inv_ref[...] = jnp.zeros_like(inv_ref)
    blocks = n // BLOCK
    for k in range(blocks):
        lo, hi = k * BLOCK, (k + 1) * BLOCK
        u_kk, inv_kk = sweep_block(work_ref[lo:hi, lo:hi])
        u_ref[lo:hi, lo:hi] = u_kk
        if k > 0:
            inv_row = hdot(inv_kk, aug_ref[lo:hi, 0:lo])
            inv_ref[lo:hi, 0:lo] = inv_row
            uinv_ref[0:lo, lo:hi] = inv_row.T
        inv_ref[lo:hi, lo:hi] = inv_kk
        uinv_ref[lo:hi, lo:hi] = inv_kk.T
        if hi < n:
            u_off = hdot(inv_kk, work_ref[lo:hi, hi:n])
            u_ref[lo:hi, hi:n] = u_off
            u_off_t = u_off.T
            work_ref[hi:n, hi:n] = work_ref[hi:n, hi:n] - hdot(u_off_t, u_off)
            aug_ref[hi:n, 0:hi] = aug_ref[hi:n, 0:hi] - hdot(u_off_t, inv_ref[lo:hi, 0:hi])


def cholesky_and_inverse(bit, mine, got):
    n = mine.shape[1]
    spec = pl.BlockSpec(memory_space=pltpu.VMEM)
    return pl.pallas_call(
        chol_kernel,
        out_shape=(jax.ShapeDtypeStruct((n, n), jnp.float32), jax.ShapeDtypeStruct((n, n), jnp.float32)),
        in_specs=[pl.BlockSpec(memory_space=pltpu.SMEM), spec, spec],
        out_specs=(spec, spec),
        scratch_shapes=[pltpu.VMEM((n, n), jnp.float32) for _ in range(3)],
    )(bit, mine, got)


def rows_kernel(a_ref, w_ref, o_ref):
    width = w_ref.shape[1]
    half = width // 2
    o_ref[:, 0:half] = hdot(a_ref[:, 0:half], w_ref[0:half, 0:half])
    o_ref[:, half:width] = hdot(a_ref[...], w_ref[:, half:width])


def rows_times(matrix, weights):
    rows, width = matrix.shape
    tile = min(rows, 512)
    return pl.pallas_call(
        rows_kernel,
        out_shape=jax.ShapeDtypeStruct((rows, weights.shape[1]), jnp.float32),
        grid=(rows // tile,),
        in_specs=[
            pl.BlockSpec((tile, width), lambda i: (i, 0)),
            pl.BlockSpec(weights.shape, lambda i: (0, 0)),
        ],
        out_specs=pl.BlockSpec((tile, weights.shape[1]), lambda i: (i, 0)),
    )(matrix, weights)


def matmul(left, right):
    return jnp.dot(left, right, precision=lax.Precision.HIGHEST, preferred_element_type=jnp.float32)


def cross(left, right):
    return lax.dot_general(
        left,
        right,
        (((0,), (0,)), ((), ())),
        precision=lax.Precision.HIGHEST,
        preferred_element_type=jnp.float32,
    )


def gram_kernel(row_count, bit_ref, a_ref, keep_ref, send_ref, acc_ref):
    step = pl.program_id(0)
    half = a_ref.shape[1] // 2

    @pl.when(step == 0)
    def _():
        acc_ref[...] = jnp.zeros_like(acc_ref)

    a = a_ref[...]
    acc_ref[:, 0:half] += cross(a, a[:, 0:half])
    acc_ref[half:, half:] += cross(a[:, half:], a[:, half:])

    @pl.when(step == pl.num_programs(0) - 1)
    def _():
        acc_ref[0:half, half:] = acc_ref[half:, 0:half].T
        top = acc_ref[0:half, :] / row_count
        bottom = acc_ref[half:, :] / row_count

        @pl.when(bit_ref[0] == 0)
        def _():
            keep_ref[...] = top
            send_ref[...] = bottom

        @pl.when(bit_ref[0] != 0)
        def _():
            keep_ref[...] = bottom
            send_ref[...] = top


def gram_halves(matrix, row_count, bit):
    rows, width = matrix.shape
    tile = min(rows, 512)
    half = jax.ShapeDtypeStruct((width // 2, width), jnp.float32)
    return pl.pallas_call(
        functools.partial(gram_kernel, row_count),
        out_shape=(half, half),
        grid=(rows // tile,),
        in_specs=[
            pl.BlockSpec(memory_space=pltpu.SMEM),
            pl.BlockSpec((tile, width), lambda i: (i, 0)),
        ],
        out_specs=(
            pl.BlockSpec((width // 2, width), lambda i: (0, 0)),
            pl.BlockSpec((width // 2, width), lambda i: (0, 0)),
        ),
        scratch_shapes=[pltpu.VMEM((width, width), jnp.float32)],
    )(bit, matrix)


def group_index(axis, shift, size):
    return (lax.axis_index(axis) >> shift) & (size - 1)


def partner_xor(value, axis, shift, offset):
    mask = offset << shift
    pairs = [(source, source ^ mask) for source in range(lax.axis_size(axis))]
    return lax.ppermute(value, axis, pairs)


def scatter_sum(value, axis, shift, size):
    height = value.shape[0] // size
    index = group_index(axis, shift, size)
    chunk = lambda j: lax.dynamic_slice_in_dim(value, j * height, height, 0)
    total = chunk(index)
    for offset in range(1, size):
        total = total + partner_xor(chunk(index ^ offset), axis, shift, offset)
    return total


def gather_all(chunk, axis, shift, size):
    height = chunk.shape[0]
    index = group_index(axis, shift, size)
    whole = jnp.zeros((height * size, chunk.shape[1]), chunk.dtype)
    whole = lax.dynamic_update_slice_in_dim(whole, chunk, index * height, 0)
    for offset in range(1, size):
        got = partner_xor(chunk, axis, shift, offset)
        whole = lax.dynamic_update_slice_in_dim(whole, got, (index ^ offset) * height, 0)
    return whole


def axis_groups(axis, first):
    bits = lax.axis_size(axis).bit_length() - 1
    groups = []
    shift = first
    while shift < bits:
        width = min(2, bits - shift)
        groups.append((axis, shift, 2**width))
        shift += width
    return groups


def on_device(response):
    row_count = response.shape[0] * lax.axis_size("inner") * lax.axis_size("wide")
    bit = jnp.reshape(lax.axis_index("wide") & 1, (1,)).astype(jnp.int32)
    keep, send = gram_halves(response, row_count, bit)
    partial_sum = keep + partner_xor(send, "wide", 0, 1)
    groups = axis_groups("inner", 0) + axis_groups("wide", 1)
    for group in groups:
        partial_sum = scatter_sum(partial_sum, *group)
    for group in reversed(groups):
        partial_sum = gather_all(partial_sum, *group)
    got = partner_xor(partial_sum, "wide", 0, 1)
    upper_factor, inverse_upper = cholesky_and_inverse(bit, partial_sum, got)
    q_rows = rows_times(response, inverse_upper)
    return (upper_factor, q_rows)


def solution(mesh):
    in_specs = (P(("inner", "wide"), None),)
    out_specs = (P(), P(("inner", "wide"), None))
    return jax.shard_map(
        on_device, mesh=mesh, in_specs=in_specs, out_specs=out_specs, check_vma=False
    )
```

```python
import functools

import jax
import jax.numpy as jnp
from jax import lax
from jax.experimental import pallas as pl
from jax.experimental.pallas import tpu as pltpu
from jax.sharding import PartitionSpec as P


BLOCK = 128
SLAB = 8


def hdot(left, right):
    return jnp.dot(left, right, precision=lax.Precision.HIGHEST, preferred_element_type=jnp.float32)


def sweep_block(diag):
    size = diag.shape[0]
    eye = (lax.broadcasted_iota(jnp.int32, (size, size), 0) == lax.broadcasted_iota(jnp.int32, (size, size), 1)).astype(jnp.float32)
    joined = jnp.concatenate([diag, eye], axis=1)
    slabs = [joined[s * SLAB:(s + 1) * SLAB] for s in range(size // SLAB)]
    rows = lax.broadcasted_iota(jnp.int32, (SLAB, 1), 0)
    for j in range(size):
        s, t = divmod(j, SLAB)
        scale = lax.rsqrt(slabs[s][t:t + 1, j:j + 1])
        top = slabs[s][t:t + 1, :] * scale
        for q in range(s + 1, len(slabs)):
            slabs[q] = slabs[q] - (slabs[q][:, j:j + 1] * scale) * top
        here = slabs[s]
        updated = here - (here[:, j:j + 1] * scale) * top
        slabs[s] = jnp.where(rows > t, updated, jnp.where(rows == t, top, here))
    joined = jnp.concatenate(slabs, axis=0)
    r = lax.broadcasted_iota(jnp.int32, (size, size), 0)
    c = lax.broadcasted_iota(jnp.int32, (size, size), 1)
    return jnp.where(c >= r, joined[:, :size], 0.0), joined[:, size:]


def chol_kernel(bit_ref, mine_ref, got_ref, u_ref, uinv_ref, work_ref, aug_ref, inv_ref):
    n = u_ref.shape[0]
    half = n // 2

    @pl.when(bit_ref[0] == 0)
    def _():
        work_ref[0:half, :] = mine_ref[...]
        work_ref[half:n, :] = got_ref[...]

    @pl.when(bit_ref[0] != 0)
    def _():
        work_ref[0:half, :] = got_ref[...]
        work_ref[half:n, :] = mine_ref[...]

    g = work_ref[...]
    work_ref[...] = (g + g.T) * 0.5
    aug_ref[...] = jnp.zeros_like(aug_ref)
    u_ref[...] = jnp.zeros_like(u_ref)
    uinv_ref[...] = jnp.zeros_like(uinv_ref)
    inv_ref[...] = jnp.zeros_like(inv_ref)
    blocks = n // BLOCK
    for k in range(blocks):
        lo, hi = k * BLOCK, (k + 1) * BLOCK
        u_kk, inv_kk = sweep_block(work_ref[lo:hi, lo:hi])
        u_ref[lo:hi, lo:hi] = u_kk
        if k > 0:
            inv_row = hdot(inv_kk, aug_ref[lo:hi, 0:lo])
            inv_ref[lo:hi, 0:lo] = inv_row
            uinv_ref[0:lo, lo:hi] = inv_row.T
        inv_ref[lo:hi, lo:hi] = inv_kk
        uinv_ref[lo:hi, lo:hi] = inv_kk.T
        if hi < n:
            u_off = hdot(inv_kk, work_ref[lo:hi, hi:n])
            u_ref[lo:hi, hi:n] = u_off
            u_off_t = u_off.T
            work_ref[hi:n, hi:n] = work_ref[hi:n, hi:n] - hdot(u_off_t, u_off)
            aug_ref[hi:n, 0:hi] = aug_ref[hi:n, 0:hi] - hdot(u_off_t, inv_ref[lo:hi, 0:hi])


def cholesky_and_inverse(bit, mine, got):
    n = mine.shape[1]
    spec = pl.BlockSpec(memory_space=pltpu.VMEM)
    return pl.pallas_call(
        chol_kernel,
        out_shape=(jax.ShapeDtypeStruct((n, n), jnp.float32), jax.ShapeDtypeStruct((n, n), jnp.float32)),
        in_specs=[pl.BlockSpec(memory_space=pltpu.SMEM), spec, spec],
        out_specs=(spec, spec),
        scratch_shapes=[pltpu.VMEM((n, n), jnp.float32) for _ in range(3)],
    )(bit, mine, got)


def rows_kernel(a_ref, w_ref, o_ref):
    width = w_ref.shape[1]
    half = width // 2
    o_ref[:, 0:half] = hdot(a_ref[:, 0:half], w_ref[0:half, 0:half])
    o_ref[:, half:width] = hdot(a_ref[...], w_ref[:, half:width])


def rows_times(matrix, weights):
    rows, width = matrix.shape
    tile = min(rows, 512)
    return pl.pallas_call(
        rows_kernel,
        out_shape=jax.ShapeDtypeStruct((rows, weights.shape[1]), jnp.float32),
        grid=(rows // tile,),
        in_specs=[
            pl.BlockSpec((tile, width), lambda i: (i, 0)),
            pl.BlockSpec(weights.shape, lambda i: (0, 0)),
        ],
        out_specs=pl.BlockSpec((tile, weights.shape[1]), lambda i: (i, 0)),
    )(matrix, weights)


def matmul(left, right):
    return jnp.dot(left, right, precision=lax.Precision.HIGHEST, preferred_element_type=jnp.float32)


def cross(left, right):
    return lax.dot_general(
        left,
        right,
        (((0,), (0,)), ((), ())),
        precision=lax.Precision.HIGHEST,
        preferred_element_type=jnp.float32,
    )


def gram_kernel(row_count, bit_ref, a_ref, keep_ref, send_ref, acc_ref):
    step = pl.program_id(0)
    half = a_ref.shape[1] // 2

    @pl.when(step == 0)
    def _():
        acc_ref[...] = jnp.zeros_like(acc_ref)

    a = a_ref[...]
    acc_ref[:, 0:half] += cross(a, a[:, 0:half])
    acc_ref[half:, half:] += cross(a[:, half:], a[:, half:])

    @pl.when(step == pl.num_programs(0) - 1)
    def _():
        acc_ref[0:half, half:] = acc_ref[half:, 0:half].T
        top = acc_ref[0:half, :] / row_count
        bottom = acc_ref[half:, :] / row_count

        @pl.when(bit_ref[0] == 0)
        def _():
            keep_ref[...] = top
            send_ref[...] = bottom

        @pl.when(bit_ref[0] != 0)
        def _():
            keep_ref[...] = bottom
            send_ref[...] = top


def gram_halves(matrix, row_count, bit):
    rows, width = matrix.shape
    tile = min(rows, 512)
    half = jax.ShapeDtypeStruct((width // 2, width), jnp.float32)
    return pl.pallas_call(
        functools.partial(gram_kernel, row_count),
        out_shape=(half, half),
        grid=(rows // tile,),
        in_specs=[
            pl.BlockSpec(memory_space=pltpu.SMEM),
            pl.BlockSpec((tile, width), lambda i: (i, 0)),
        ],
        out_specs=(
            pl.BlockSpec((width // 2, width), lambda i: (0, 0)),
            pl.BlockSpec((width // 2, width), lambda i: (0, 0)),
        ),
        scratch_shapes=[pltpu.VMEM((width, width), jnp.float32)],
    )(bit, matrix)


def group_index(axis, shift, size):
    return (lax.axis_index(axis) >> shift) & (size - 1)


def partner_xor(value, axis, shift, offset):
    mask = offset << shift
    pairs = [(source, source ^ mask) for source in range(lax.axis_size(axis))]
    return lax.ppermute(value, axis, pairs)


def scatter_sum(addends, axis, shift, size):
    height = addends[0].shape[0] // size
    index = group_index(axis, shift, size)

    def chunk(j):
        parts = [lax.dynamic_slice_in_dim(part, j * height, height, 0) for part in addends]
        return functools.reduce(jnp.add, parts)

    total = chunk(index)
    for offset in range(1, size):
        total = total + partner_xor(chunk(index ^ offset), axis, shift, offset)
    return total


def gather_all(chunk, axis, shift, size):
    height = chunk.shape[0]
    index = group_index(axis, shift, size)
    whole = jnp.zeros((height * size, chunk.shape[1]), chunk.dtype)
    whole = lax.dynamic_update_slice_in_dim(whole, chunk, index * height, 0)
    for offset in range(1, size):
        got = partner_xor(chunk, axis, shift, offset)
        whole = lax.dynamic_update_slice_in_dim(whole, got, (index ^ offset) * height, 0)
    return whole


def axis_groups(axis, first):
    bits = lax.axis_size(axis).bit_length() - 1
    groups = []
    shift = first
    while shift < bits:
        width = min(2, bits - shift)
        groups.append((axis, shift, 2**width))
        shift += width
    return groups


def on_device(response):
    row_count = response.shape[0] * lax.axis_size("inner") * lax.axis_size("wide")
    bit = jnp.reshape(lax.axis_index("wide") & 1, (1,)).astype(jnp.int32)
    keep, send = gram_halves(response, row_count, bit)
    addends = [keep, partner_xor(send, "wide", 0, 1)]
    groups = axis_groups("inner", 0) + axis_groups("wide", 1)
    for group in groups:
        partial_sum = scatter_sum(addends, *group)
        addends = [partial_sum]
    for group in reversed(groups):
        partial_sum = gather_all(partial_sum, *group)
    got = partner_xor(partial_sum, "wide", 0, 1)
    upper_factor, inverse_upper = cholesky_and_inverse(bit, partial_sum, got)
    q_rows = rows_times(response, inverse_upper)
    return (upper_factor, q_rows)


def solution(mesh):
    in_specs = (P(("inner", "wide"), None),)
    out_specs = (P(), P(("inner", "wide"), None))
    return jax.shard_map(
        on_device, mesh=mesh, in_specs=in_specs, out_specs=out_specs, check_vma=False
    )
```

```python
import jax
import jax.numpy as jnp
from jax import lax
from jax.experimental import pallas as pl
from jax.experimental.pallas import tpu as pltpu
from jax.sharding import PartitionSpec as P


BLOCK = 128
SLAB = 8


def hdot(left, right):
    return jnp.dot(left, right, precision=lax.Precision.HIGHEST, preferred_element_type=jnp.float32)


def sweep_block(diag):
    size = diag.shape[0]
    eye = (lax.broadcasted_iota(jnp.int32, (size, size), 0) == lax.broadcasted_iota(jnp.int32, (size, size), 1)).astype(jnp.float32)
    joined = jnp.concatenate([diag, eye], axis=1)
    slabs = [joined[s * SLAB:(s + 1) * SLAB] for s in range(size // SLAB)]
    rows = lax.broadcasted_iota(jnp.int32, (SLAB, 1), 0)
    for j in range(size):
        s, t = divmod(j, SLAB)
        scale = lax.rsqrt(slabs[s][t:t + 1, j:j + 1])
        top = slabs[s][t:t + 1, :] * scale
        for q in range(s + 1, len(slabs)):
            slabs[q] = slabs[q] - (slabs[q][:, j:j + 1] * scale) * top
        here = slabs[s]
        updated = here - (here[:, j:j + 1] * scale) * top
        slabs[s] = jnp.where(rows > t, updated, jnp.where(rows == t, top, here))
    joined = jnp.concatenate(slabs, axis=0)
    r = lax.broadcasted_iota(jnp.int32, (size, size), 0)
    c = lax.broadcasted_iota(jnp.int32, (size, size), 1)
    return jnp.where(c >= r, joined[:, :size], 0.0), joined[:, size:]


def chol_kernel(g_ref, u_ref, uinv_ref, work_ref, aug_ref, inv_ref):
    n = g_ref.shape[0]
    g = g_ref[...]
    work_ref[...] = (g + g.T) * 0.5
    aug_ref[...] = jnp.zeros_like(aug_ref)
    u_ref[...] = jnp.zeros_like(u_ref)
    uinv_ref[...] = jnp.zeros_like(uinv_ref)
    inv_ref[...] = jnp.zeros_like(inv_ref)
    blocks = n // BLOCK
    for k in range(blocks):
        lo, hi = k * BLOCK, (k + 1) * BLOCK
        u_kk, inv_kk = sweep_block(work_ref[lo:hi, lo:hi])
        u_ref[lo:hi, lo:hi] = u_kk
        if k > 0:
            inv_row = hdot(inv_kk, aug_ref[lo:hi, 0:lo])
            inv_ref[lo:hi, 0:lo] = inv_row
            uinv_ref[0:lo, lo:hi] = inv_row.T
        inv_ref[lo:hi, lo:hi] = inv_kk
        uinv_ref[lo:hi, lo:hi] = inv_kk.T
        if hi < n:
            u_off = hdot(inv_kk, work_ref[lo:hi, hi:n])
            u_ref[lo:hi, hi:n] = u_off
            u_off_t = u_off.T
            work_ref[hi:n, hi:n] = work_ref[hi:n, hi:n] - hdot(u_off_t, u_off)
            aug_ref[hi:n, 0:hi] = aug_ref[hi:n, 0:hi] - hdot(u_off_t, inv_ref[lo:hi, 0:hi])


def cholesky_and_inverse(gram_matrix):
    n = gram_matrix.shape[0]
    spec = pl.BlockSpec(memory_space=pltpu.VMEM)
    return pl.pallas_call(
        chol_kernel,
        out_shape=(jax.ShapeDtypeStruct((n, n), jnp.float32), jax.ShapeDtypeStruct((n, n), jnp.float32)),
        in_specs=[spec],
        out_specs=(spec, spec),
        scratch_shapes=[pltpu.VMEM((n, n), jnp.float32) for _ in range(3)],
    )(gram_matrix)


def rows_kernel(a_ref, w_ref, o_ref):
    width = w_ref.shape[1]
    half = width // 2
    o_ref[:, 0:half] = hdot(a_ref[:, 0:half], w_ref[0:half, 0:half])
    o_ref[:, half:width] = hdot(a_ref[...], w_ref[:, half:width])


def rows_times(matrix, weights):
    rows, width = matrix.shape
    tile = min(rows, 512)
    return pl.pallas_call(
        rows_kernel,
        out_shape=jax.ShapeDtypeStruct((rows, weights.shape[1]), jnp.float32),
        grid=(rows // tile,),
        in_specs=[
            pl.BlockSpec((tile, width), lambda i: (i, 0)),
            pl.BlockSpec(weights.shape, lambda i: (0, 0)),
        ],
        out_specs=pl.BlockSpec((tile, weights.shape[1]), lambda i: (i, 0)),
    )(matrix, weights)


def matmul(left, right):
    return jnp.dot(left, right, precision=lax.Precision.HIGHEST, preferred_element_type=jnp.float32)


def gram_of(matrix):
    return lax.dot_general(
        matrix,
        matrix,
        (((0,), (0,)), ((), ())),
        precision=lax.Precision.HIGHEST,
        preferred_element_type=jnp.float32,
    )


def group_index(axis, shift, size):
    return (lax.axis_index(axis) >> shift) & (size - 1)


def partner_xor(value, axis, shift, offset):
    mask = offset << shift
    pairs = [(source, source ^ mask) for source in range(lax.axis_size(axis))]
    return lax.ppermute(value, axis, pairs)


def scatter_sum(value, axis, shift, size):
    height = value.shape[0] // size
    index = group_index(axis, shift, size)
    chunk = lambda j: lax.dynamic_slice_in_dim(value, j * height, height, 0)
    total = chunk(index)
    for offset in range(1, size):
        total = total + partner_xor(chunk(index ^ offset), axis, shift, offset)
    return total


def gather_all(chunk, axis, shift, size):
    height = chunk.shape[0]
    index = group_index(axis, shift, size)
    whole = jnp.zeros((height * size, chunk.shape[1]), chunk.dtype)
    whole = lax.dynamic_update_slice_in_dim(whole, chunk, index * height, 0)
    for offset in range(1, size):
        got = partner_xor(chunk, axis, shift, offset)
        whole = lax.dynamic_update_slice_in_dim(whole, got, (index ^ offset) * height, 0)
    return whole


def axis_groups(axis, first):
    bits = lax.axis_size(axis).bit_length() - 1
    groups = []
    shift = first
    while shift < bits:
        width = min(2, bits - shift)
        groups.append((axis, shift, 2**width))
        shift += width
    return groups


def all_sum(gram_matrix):
    groups = axis_groups("inner", 0) + axis_groups("wide", 1)
    for group in groups:
        gram_matrix = scatter_sum(gram_matrix, *group)
    gram_matrix = gram_matrix + partner_xor(gram_matrix, "wide", 0, 1)
    for group in reversed(groups):
        gram_matrix = gather_all(gram_matrix, *group)
    return gram_matrix


def on_device(response):
    row_count = response.shape[0] * lax.axis_size("inner") * lax.axis_size("wide")
    gram_matrix = gram_of(response) / row_count
    gram_matrix = all_sum(gram_matrix)
    upper_factor, inverse_upper = cholesky_and_inverse(gram_matrix)
    q_rows = rows_times(response, inverse_upper)
    return (upper_factor, q_rows)


def solution(mesh):
    in_specs = (P(("inner", "wide"), None),)
    out_specs = (P(), P(("inner", "wide"), None))
    return jax.shard_map(
        on_device, mesh=mesh, in_specs=in_specs, out_specs=out_specs, check_vma=False
    )
```

```python
import functools

import jax
import jax.numpy as jnp
from jax import lax
from jax.experimental import pallas as pl
from jax.experimental.pallas import tpu as pltpu
from jax.sharding import PartitionSpec as P


BLOCK = 128
SLAB = 8


def hdot(left, right):
    return jnp.dot(left, right, precision=lax.Precision.HIGHEST, preferred_element_type=jnp.float32)


def sweep_block(diag):
    size = diag.shape[0]
    eye = (lax.broadcasted_iota(jnp.int32, (size, size), 0) == lax.broadcasted_iota(jnp.int32, (size, size), 1)).astype(jnp.float32)
    joined = jnp.concatenate([diag, eye], axis=1)
    slabs = [joined[s * SLAB:(s + 1) * SLAB] for s in range(size // SLAB)]
    rows = lax.broadcasted_iota(jnp.int32, (SLAB, 1), 0)
    for j in range(size):
        s, t = divmod(j, SLAB)
        scale = lax.rsqrt(slabs[s][t:t + 1, j:j + 1])
        top = slabs[s][t:t + 1, :] * scale
        for q in range(s + 1, len(slabs)):
            slabs[q] = slabs[q] - (slabs[q][:, j:j + 1] * scale) * top
        here = slabs[s]
        updated = here - (here[:, j:j + 1] * scale) * top
        slabs[s] = jnp.where(rows > t, updated, jnp.where(rows == t, top, here))
    joined = jnp.concatenate(slabs, axis=0)
    r = lax.broadcasted_iota(jnp.int32, (size, size), 0)
    c = lax.broadcasted_iota(jnp.int32, (size, size), 1)
    return jnp.where(c >= r, joined[:, :size], 0.0), joined[:, size:]


def chol_kernel(bit_ref, mine_ref, got_ref, u_ref, uinv_ref, work_ref, aug_ref, inv_ref):
    n = u_ref.shape[0]
    half = n // 2

    @pl.when(bit_ref[0] == 0)
    def _():
        work_ref[0:half, :] = mine_ref[...]
        work_ref[half:n, :] = got_ref[...]

    @pl.when(bit_ref[0] != 0)
    def _():
        work_ref[0:half, :] = got_ref[...]
        work_ref[half:n, :] = mine_ref[...]

    aug_ref[...] = jnp.zeros_like(aug_ref)
    blocks = n // BLOCK
    for k in range(blocks):
        lo, hi = k * BLOCK, (k + 1) * BLOCK
        if hi < n:
            u_ref[hi:n, lo:hi] = jnp.zeros((n - hi, BLOCK), jnp.float32)
            uinv_ref[hi:n, lo:hi] = jnp.zeros((n - hi, BLOCK), jnp.float32)
        u_kk, inv_kk = sweep_block(work_ref[lo:hi, lo:hi])
        u_ref[lo:hi, lo:hi] = u_kk
        if k > 0:
            inv_row = hdot(inv_kk, aug_ref[lo:hi, 0:lo])
            inv_ref[lo:hi, 0:lo] = inv_row
            uinv_ref[0:lo, lo:hi] = inv_row.T
        inv_ref[lo:hi, lo:hi] = inv_kk
        uinv_ref[lo:hi, lo:hi] = inv_kk.T
        if hi < n:
            u_off = hdot(inv_kk, work_ref[lo:hi, hi:n])
            u_ref[lo:hi, hi:n] = u_off
            u_off_t = u_off.T
            work_ref[hi:n, hi:n] = work_ref[hi:n, hi:n] - hdot(u_off_t, u_off)
            aug_ref[hi:n, 0:hi] = aug_ref[hi:n, 0:hi] - hdot(u_off_t, inv_ref[lo:hi, 0:hi])


def cholesky_and_inverse(bit, mine, got):
    n = mine.shape[1]
    spec = pl.BlockSpec(memory_space=pltpu.VMEM)
    return pl.pallas_call(
        chol_kernel,
        out_shape=(jax.ShapeDtypeStruct((n, n), jnp.float32), jax.ShapeDtypeStruct((n, n), jnp.float32)),
        in_specs=[pl.BlockSpec(memory_space=pltpu.SMEM), spec, spec],
        out_specs=(spec, spec),
        scratch_shapes=[pltpu.VMEM((n, n), jnp.float32) for _ in range(3)],
    )(bit, mine, got)


def rows_kernel(a_ref, w_ref, o_ref):
    width = w_ref.shape[1]
    half = width // 2
    o_ref[:, 0:half] = hdot(a_ref[:, 0:half], w_ref[0:half, 0:half])
    o_ref[:, half:width] = hdot(a_ref[...], w_ref[:, half:width])


def rows_times(matrix, weights):
    rows, width = matrix.shape
    tile = min(rows, 512)
    return pl.pallas_call(
        rows_kernel,
        out_shape=jax.ShapeDtypeStruct((rows, weights.shape[1]), jnp.float32),
        grid=(rows // tile,),
        in_specs=[
            pl.BlockSpec((tile, width), lambda i: (i, 0)),
            pl.BlockSpec(weights.shape, lambda i: (0, 0)),
        ],
        out_specs=pl.BlockSpec((tile, weights.shape[1]), lambda i: (i, 0)),
    )(matrix, weights)


def matmul(left, right):
    return jnp.dot(left, right, precision=lax.Precision.HIGHEST, preferred_element_type=jnp.float32)


def cross(left, right):
    return lax.dot_general(
        left,
        right,
        (((0,), (0,)), ((), ())),
        precision=lax.Precision.HIGHEST,
        preferred_element_type=jnp.float32,
    )


def gram_kernel(row_count, bit_ref, a_ref, keep_ref, send_ref, acc_ref):
    step = pl.program_id(0)
    half = a_ref.shape[1] // 2

    @pl.when(step == 0)
    def _():
        acc_ref[...] = jnp.zeros_like(acc_ref)

    a = a_ref[...]
    acc_ref[:, 0:half] += cross(a, a[:, 0:half])
    acc_ref[half:, half:] += cross(a[:, half:], a[:, half:])

    @pl.when(step == pl.num_programs(0) - 1)
    def _():
        acc_ref[0:half, half:] = acc_ref[half:, 0:half].T
        top = acc_ref[0:half, :] / row_count
        bottom = acc_ref[half:, :] / row_count

        @pl.when(bit_ref[0] == 0)
        def _():
            keep_ref[...] = top
            send_ref[...] = bottom

        @pl.when(bit_ref[0] != 0)
        def _():
            keep_ref[...] = bottom
            send_ref[...] = top


def gram_halves(matrix, row_count, bit):
    rows, width = matrix.shape
    tile = min(rows, 512)
    half = jax.ShapeDtypeStruct((width // 2, width), jnp.float32)
    return pl.pallas_call(
        functools.partial(gram_kernel, row_count),
        out_shape=(half, half),
        grid=(rows // tile,),
        in_specs=[
            pl.BlockSpec(memory_space=pltpu.SMEM),
            pl.BlockSpec((tile, width), lambda i: (i, 0)),
        ],
        out_specs=(
            pl.BlockSpec((width // 2, width), lambda i: (0, 0)),
            pl.BlockSpec((width // 2, width), lambda i: (0, 0)),
        ),
        scratch_shapes=[pltpu.VMEM((width, width), jnp.float32)],
    )(bit, matrix)


def group_index(axis, shift, size):
    return (lax.axis_index(axis) >> shift) & (size - 1)


def partner_xor(value, axis, shift, offset):
    mask = offset << shift
    pairs = [(source, source ^ mask) for source in range(lax.axis_size(axis))]
    return lax.ppermute(value, axis, pairs)


def scatter_sum(value, axis, shift, size):
    height = value.shape[0] // size
    index = group_index(axis, shift, size)
    chunk = lambda j: lax.dynamic_slice_in_dim(value, j * height, height, 0)
    total = chunk(index)
    for offset in range(1, size):
        total = total + partner_xor(chunk(index ^ offset), axis, shift, offset)
    return total


def gather_all(chunk, axis, shift, size):
    height = chunk.shape[0]
    index = group_index(axis, shift, size)
    whole = jnp.zeros((height * size, chunk.shape[1]), chunk.dtype)
    whole = lax.dynamic_update_slice_in_dim(whole, chunk, index * height, 0)
    for offset in range(1, size):
        got = partner_xor(chunk, axis, shift, offset)
        whole = lax.dynamic_update_slice_in_dim(whole, got, (index ^ offset) * height, 0)
    return whole


def axis_groups(axis, first):
    bits = lax.axis_size(axis).bit_length() - 1
    groups = []
    shift = first
    while shift < bits:
        width = min(2, bits - shift)
        groups.append((axis, shift, 2**width))
        shift += width
    return groups


def on_device(response):
    row_count = response.shape[0] * lax.axis_size("inner") * lax.axis_size("wide")
    bit = jnp.reshape(lax.axis_index("wide") & 1, (1,)).astype(jnp.int32)
    keep, send = gram_halves(response, row_count, bit)
    partial_sum = keep + partner_xor(send, "wide", 0, 1)
    groups = axis_groups("inner", 0) + axis_groups("wide", 1)
    for group in groups:
        partial_sum = scatter_sum(partial_sum, *group)
    for group in reversed(groups):
        partial_sum = gather_all(partial_sum, *group)
    got = partner_xor(partial_sum, "wide", 0, 1)
    upper_factor, inverse_upper = cholesky_and_inverse(bit, partial_sum, got)
    q_rows = rows_times(response, inverse_upper)
    return (upper_factor, q_rows)


def solution(mesh):
    in_specs = (P(("inner", "wide"), None),)
    out_specs = (P(), P(("inner", "wide"), None))
    return jax.shard_map(
        on_device, mesh=mesh, in_specs=in_specs, out_specs=out_specs, check_vma=False
    )
```

```python
import functools

import jax
import jax.numpy as jnp
from jax import lax
from jax.experimental import pallas as pl
from jax.experimental.pallas import tpu as pltpu
from jax.sharding import PartitionSpec as P


BLOCK = 128
SLAB = 8


STACK = 5 * BLOCK


def lower_stacks(acc_ref):
    b = BLOCK
    first = jnp.concatenate([acc_ref[:, 0:b], acc_ref[b:2 * b, b:2 * b]], axis=0)
    second = jnp.concatenate(
        [acc_ref[2 * b:4 * b, b:2 * b], acc_ref[2 * b:4 * b, 2 * b:3 * b], acc_ref[3 * b:4 * b, 3 * b:4 * b]], axis=0
    )
    return first, second


def fill_gram(work_ref, first_ref, second_ref):
    b = BLOCK
    work_ref[:, 0:b] = first_ref[0:4 * b, :]
    work_ref[b:2 * b, b:2 * b] = first_ref[4 * b:5 * b, :]
    work_ref[2 * b:4 * b, b:2 * b] = second_ref[0:2 * b, :]
    work_ref[2 * b:4 * b, 2 * b:3 * b] = second_ref[2 * b:4 * b, :]
    work_ref[3 * b:4 * b, 3 * b:4 * b] = second_ref[4 * b:5 * b, :]
    for i in range(4):
        for j in range(i + 1, 4):
            work_ref[i * b:(i + 1) * b, j * b:(j + 1) * b] = work_ref[j * b:(j + 1) * b, i * b:(i + 1) * b].T


def hdot(left, right):
    return jnp.dot(left, right, precision=lax.Precision.HIGHEST, preferred_element_type=jnp.float32)


def sweep_block(diag):
    size = diag.shape[0]
    eye = (lax.broadcasted_iota(jnp.int32, (size, size), 0) == lax.broadcasted_iota(jnp.int32, (size, size), 1)).astype(jnp.float32)
    joined = jnp.concatenate([diag, eye], axis=1)
    slabs = [joined[s * SLAB:(s + 1) * SLAB] for s in range(size // SLAB)]
    rows = lax.broadcasted_iota(jnp.int32, (SLAB, 1), 0)
    for j in range(size):
        s, t = divmod(j, SLAB)
        scale = lax.rsqrt(slabs[s][t:t + 1, j:j + 1])
        top = slabs[s][t:t + 1, :] * scale
        for q in range(s + 1, len(slabs)):
            slabs[q] = slabs[q] - (slabs[q][:, j:j + 1] * scale) * top
        here = slabs[s]
        updated = here - (here[:, j:j + 1] * scale) * top
        slabs[s] = jnp.where(rows > t, updated, jnp.where(rows == t, top, here))
    joined = jnp.concatenate(slabs, axis=0)
    r = lax.broadcasted_iota(jnp.int32, (size, size), 0)
    c = lax.broadcasted_iota(jnp.int32, (size, size), 1)
    return jnp.where(c >= r, joined[:, :size], 0.0), joined[:, size:]


def chol_kernel(bit_ref, mine_ref, got_ref, u_ref, uinv_ref, work_ref, aug_ref, inv_ref):
    n = u_ref.shape[0]

    @pl.when(bit_ref[0] == 0)
    def _():
        fill_gram(work_ref, mine_ref, got_ref)

    @pl.when(bit_ref[0] != 0)
    def _():
        fill_gram(work_ref, got_ref, mine_ref)

    aug_ref[...] = jnp.zeros_like(aug_ref)
    blocks = n // BLOCK
    for k in range(blocks):
        lo, hi = k * BLOCK, (k + 1) * BLOCK
        if hi < n:
            u_ref[hi:n, lo:hi] = jnp.zeros((n - hi, BLOCK), jnp.float32)
            uinv_ref[hi:n, lo:hi] = jnp.zeros((n - hi, BLOCK), jnp.float32)
        u_kk, inv_kk = sweep_block(work_ref[lo:hi, lo:hi])
        u_ref[lo:hi, lo:hi] = u_kk
        if k > 0:
            inv_row = hdot(inv_kk, aug_ref[lo:hi, 0:lo])
            inv_ref[lo:hi, 0:lo] = inv_row
            uinv_ref[0:lo, lo:hi] = inv_row.T
        inv_ref[lo:hi, lo:hi] = inv_kk
        uinv_ref[lo:hi, lo:hi] = inv_kk.T
        if hi < n:
            u_off = hdot(inv_kk, work_ref[lo:hi, hi:n])
            u_ref[lo:hi, hi:n] = u_off
            u_off_t = u_off.T
            work_ref[hi:n, hi:n] = work_ref[hi:n, hi:n] - hdot(u_off_t, u_off)
            aug_ref[hi:n, 0:hi] = aug_ref[hi:n, 0:hi] - hdot(u_off_t, inv_ref[lo:hi, 0:hi])


def cholesky_and_inverse(bit, mine, got):
    n = 4 * BLOCK
    spec = pl.BlockSpec(memory_space=pltpu.VMEM)
    return pl.pallas_call(
        chol_kernel,
        out_shape=(jax.ShapeDtypeStruct((n, n), jnp.float32), jax.ShapeDtypeStruct((n, n), jnp.float32)),
        in_specs=[pl.BlockSpec(memory_space=pltpu.SMEM), spec, spec],
        out_specs=(spec, spec),
        scratch_shapes=[pltpu.VMEM((n, n), jnp.float32) for _ in range(3)],
    )(bit, mine, got)


def rows_kernel(a_ref, w_ref, o_ref):
    width = w_ref.shape[1]
    half = width // 2
    o_ref[:, 0:half] = hdot(a_ref[:, 0:half], w_ref[0:half, 0:half])
    o_ref[:, half:width] = hdot(a_ref[...], w_ref[:, half:width])


def rows_times(matrix, weights):
    rows, width = matrix.shape
    tile = min(rows, 512)
    return pl.pallas_call(
        rows_kernel,
        out_shape=jax.ShapeDtypeStruct((rows, weights.shape[1]), jnp.float32),
        grid=(rows // tile,),
        in_specs=[
            pl.BlockSpec((tile, width), lambda i: (i, 0)),
            pl.BlockSpec(weights.shape, lambda i: (0, 0)),
        ],
        out_specs=pl.BlockSpec((tile, weights.shape[1]), lambda i: (i, 0)),
    )(matrix, weights)


def matmul(left, right):
    return jnp.dot(left, right, precision=lax.Precision.HIGHEST, preferred_element_type=jnp.float32)


def cross(left, right):
    return lax.dot_general(
        left,
        right,
        (((0,), (0,)), ((), ())),
        precision=lax.Precision.HIGHEST,
        preferred_element_type=jnp.float32,
    )


def gram_kernel(row_count, bit_ref, a_ref, keep_ref, send_ref, acc_ref):
    step = pl.program_id(0)
    half = a_ref.shape[1] // 2

    @pl.when(step == 0)
    def _():
        acc_ref[...] = jnp.zeros_like(acc_ref)

    a = a_ref[...]
    acc_ref[:, 0:half] += cross(a, a[:, 0:half])
    acc_ref[half:, half:] += cross(a[:, half:], a[:, half:])

    @pl.when(step == pl.num_programs(0) - 1)
    def _():
        first, second = lower_stacks(acc_ref)
        first = first / row_count
        second = second / row_count

        @pl.when(bit_ref[0] == 0)
        def _():
            keep_ref[...] = first
            send_ref[...] = second

        @pl.when(bit_ref[0] != 0)
        def _():
            keep_ref[...] = second
            send_ref[...] = first


def gram_halves(matrix, row_count, bit):
    rows, width = matrix.shape
    tile = min(rows, 512)
    half = jax.ShapeDtypeStruct((STACK, BLOCK), jnp.float32)
    return pl.pallas_call(
        functools.partial(gram_kernel, row_count),
        out_shape=(half, half),
        grid=(rows // tile,),
        in_specs=[
            pl.BlockSpec(memory_space=pltpu.SMEM),
            pl.BlockSpec((tile, width), lambda i: (i, 0)),
        ],
        out_specs=(
            pl.BlockSpec((STACK, BLOCK), lambda i: (0, 0)),
            pl.BlockSpec((STACK, BLOCK), lambda i: (0, 0)),
        ),
        scratch_shapes=[pltpu.VMEM((width, width), jnp.float32)],
    )(bit, matrix)


def group_index(axis, shift, size):
    return (lax.axis_index(axis) >> shift) & (size - 1)


def partner_xor(value, axis, shift, offset):
    mask = offset << shift
    pairs = [(source, source ^ mask) for source in range(lax.axis_size(axis))]
    return lax.ppermute(value, axis, pairs)


def scatter_sum(value, axis, shift, size):
    height = value.shape[0] // size
    index = group_index(axis, shift, size)
    chunk = lambda j: lax.dynamic_slice_in_dim(value, j * height, height, 0)
    total = chunk(index)
    for offset in range(1, size):
        total = total + partner_xor(chunk(index ^ offset), axis, shift, offset)
    return total


def gather_all(chunk, axis, shift, size):
    height = chunk.shape[0]
    index = group_index(axis, shift, size)
    whole = jnp.zeros((height * size, chunk.shape[1]), chunk.dtype)
    whole = lax.dynamic_update_slice_in_dim(whole, chunk, index * height, 0)
    for offset in range(1, size):
        got = partner_xor(chunk, axis, shift, offset)
        whole = lax.dynamic_update_slice_in_dim(whole, got, (index ^ offset) * height, 0)
    return whole


def axis_groups(axis, first):
    bits = lax.axis_size(axis).bit_length() - 1
    groups = []
    shift = first
    while shift < bits:
        width = min(2, bits - shift)
        groups.append((axis, shift, 2**width))
        shift += width
    return groups


def on_device(response):
    row_count = response.shape[0] * lax.axis_size("inner") * lax.axis_size("wide")
    bit = jnp.reshape(lax.axis_index("wide") & 1, (1,)).astype(jnp.int32)
    keep, send = gram_halves(response, row_count, bit)
    partial_sum = keep + partner_xor(send, "wide", 0, 1)
    groups = axis_groups("inner", 0) + axis_groups("wide", 1)
    for group in groups:
        partial_sum = scatter_sum(partial_sum, *group)
    for group in reversed(groups):
        partial_sum = gather_all(partial_sum, *group)
    got = partner_xor(partial_sum, "wide", 0, 1)
    upper_factor, inverse_upper = cholesky_and_inverse(bit, partial_sum, got)
    q_rows = rows_times(response, inverse_upper)
    return (upper_factor, q_rows)


def solution(mesh):
    in_specs = (P(("inner", "wide"), None),)
    out_specs = (P(), P(("inner", "wide"), None))
    return jax.shard_map(
        on_device, mesh=mesh, in_specs=in_specs, out_specs=out_specs, check_vma=False
    )
```

```python
import functools

import jax
import jax.numpy as jnp
from jax import lax
from jax.experimental import pallas as pl
from jax.experimental.pallas import tpu as pltpu
from jax.sharding import PartitionSpec as P


BLOCK = 128
SLAB = 8


STACK = 5 * BLOCK


def lower_stacks(acc_ref):
    b = BLOCK
    first = jnp.concatenate([acc_ref[:, 0:b], acc_ref[b:2 * b, b:2 * b]], axis=0)
    second = jnp.concatenate(
        [acc_ref[2 * b:4 * b, b:2 * b], acc_ref[2 * b:4 * b, 2 * b:3 * b], acc_ref[3 * b:4 * b, 3 * b:4 * b]], axis=0
    )
    return first, second


def fill_gram(work_ref, first_ref, second_ref):
    b = BLOCK
    work_ref[:, 0:b] = first_ref[0:4 * b, :]
    work_ref[b:2 * b, b:2 * b] = first_ref[4 * b:5 * b, :]
    work_ref[2 * b:4 * b, b:2 * b] = second_ref[0:2 * b, :]
    work_ref[2 * b:4 * b, 2 * b:3 * b] = second_ref[2 * b:4 * b, :]
    work_ref[3 * b:4 * b, 3 * b:4 * b] = second_ref[4 * b:5 * b, :]
    for i in range(4):
        for j in range(i + 1, 4):
            work_ref[i * b:(i + 1) * b, j * b:(j + 1) * b] = work_ref[j * b:(j + 1) * b, i * b:(i + 1) * b].T


def hdot(left, right):
    return jnp.dot(left, right, precision=lax.Precision.HIGHEST, preferred_element_type=jnp.float32)


def sweep_block(diag):
    size = diag.shape[0]
    eye = (lax.broadcasted_iota(jnp.int32, (size, size), 0) == lax.broadcasted_iota(jnp.int32, (size, size), 1)).astype(jnp.float32)
    joined = jnp.concatenate([diag, eye], axis=1)
    slabs = [joined[s * SLAB:(s + 1) * SLAB] for s in range(size // SLAB)]
    rows = lax.broadcasted_iota(jnp.int32, (SLAB, 1), 0)
    for j in range(size):
        s, t = divmod(j, SLAB)
        scale = lax.rsqrt(slabs[s][t:t + 1, j:j + 1])
        top = slabs[s][t:t + 1, :] * scale
        for q in range(s + 1, len(slabs)):
            slabs[q] = slabs[q] - (slabs[q][:, j:j + 1] * scale) * top
        here = slabs[s]
        updated = here - (here[:, j:j + 1] * scale) * top
        slabs[s] = jnp.where(rows > t, updated, jnp.where(rows == t, top, here))
    joined = jnp.concatenate(slabs, axis=0)
    r = lax.broadcasted_iota(jnp.int32, (size, size), 0)
    c = lax.broadcasted_iota(jnp.int32, (size, size), 1)
    return jnp.where(c >= r, joined[:, :size], 0.0), joined[:, size:]


def chol_kernel(bit_ref, mine_ref, got_ref, u_ref, uinv_ref, work_ref, aug_ref, inv_ref):
    n = u_ref.shape[0]

    @pl.when(bit_ref[0] == 0)
    def _():
        fill_gram(work_ref, mine_ref, got_ref)

    @pl.when(bit_ref[0] != 0)
    def _():
        fill_gram(work_ref, got_ref, mine_ref)

    aug_ref[...] = jnp.zeros_like(aug_ref)
    blocks = n // BLOCK
    for k in range(blocks):
        lo, hi = k * BLOCK, (k + 1) * BLOCK
        if hi < n:
            u_ref[hi:n, lo:hi] = jnp.zeros((n - hi, BLOCK), jnp.float32)
            uinv_ref[hi:n, lo:hi] = jnp.zeros((n - hi, BLOCK), jnp.float32)
        u_kk, inv_kk = sweep_block(work_ref[lo:hi, lo:hi])
        u_ref[lo:hi, lo:hi] = u_kk
        if k > 0:
            inv_row = hdot(inv_kk, aug_ref[lo:hi, 0:lo])
            inv_ref[lo:hi, 0:lo] = inv_row
            uinv_ref[0:lo, lo:hi] = inv_row.T
        inv_ref[lo:hi, lo:hi] = inv_kk
        uinv_ref[lo:hi, lo:hi] = inv_kk.T
        if hi < n:
            u_off = hdot(inv_kk, work_ref[lo:hi, hi:n])
            u_ref[lo:hi, hi:n] = u_off
            u_off_t = u_off.T
            work_ref[hi:n, hi:n] = work_ref[hi:n, hi:n] - hdot(u_off_t, u_off)
            aug_ref[hi:n, 0:hi] = aug_ref[hi:n, 0:hi] - hdot(u_off_t, inv_ref[lo:hi, 0:hi])


def cholesky_and_inverse(bit, mine, got):
    n = 4 * BLOCK
    spec = pl.BlockSpec(memory_space=pltpu.VMEM)
    return pl.pallas_call(
        chol_kernel,
        out_shape=(jax.ShapeDtypeStruct((n, n), jnp.float32), jax.ShapeDtypeStruct((n, n), jnp.float32)),
        in_specs=[pl.BlockSpec(memory_space=pltpu.SMEM), spec, spec],
        out_specs=(spec, spec),
        scratch_shapes=[pltpu.VMEM((n, n), jnp.float32) for _ in range(3)],
    )(bit, mine, got)


def rows_kernel(a_ref, w_ref, o_ref):
    width = w_ref.shape[1]
    half = width // 2
    o_ref[:, 0:half] = hdot(a_ref[:, 0:half], w_ref[0:half, 0:half])
    o_ref[:, half:width] = hdot(a_ref[...], w_ref[:, half:width])


def rows_times(matrix, weights):
    rows, width = matrix.shape
    tile = min(rows, 512)
    return pl.pallas_call(
        rows_kernel,
        out_shape=jax.ShapeDtypeStruct((rows, weights.shape[1]), jnp.float32),
        grid=(rows // tile,),
        in_specs=[
            pl.BlockSpec((tile, width), lambda i: (i, 0)),
            pl.BlockSpec(weights.shape, lambda i: (0, 0)),
        ],
        out_specs=pl.BlockSpec((tile, weights.shape[1]), lambda i: (i, 0)),
    )(matrix, weights)


def matmul(left, right):
    return jnp.dot(left, right, precision=lax.Precision.HIGHEST, preferred_element_type=jnp.float32)


def cross(left, right):
    return lax.dot_general(
        left,
        right,
        (((0,), (0,)), ((), ())),
        precision=lax.Precision.HIGHEST,
        preferred_element_type=jnp.float32,
    )


def gram_kernel(row_count, bit_ref, a_ref, keep_ref, send_ref, acc_ref):
    step = pl.program_id(0)
    half = a_ref.shape[1] // 2

    @pl.when(step == 0)
    def _():
        acc_ref[...] = jnp.zeros_like(acc_ref)

    a = a_ref[...]
    acc_ref[:, 0:half] += cross(a, a[:, 0:half])
    acc_ref[half:, half:] += cross(a[:, half:], a[:, half:])

    @pl.when(step == pl.num_programs(0) - 1)
    def _():
        first, second = lower_stacks(acc_ref)
        first = first / row_count
        second = second / row_count

        @pl.when(bit_ref[0] == 0)
        def _():
            keep_ref[...] = first
            send_ref[...] = second

        @pl.when(bit_ref[0] != 0)
        def _():
            keep_ref[...] = second
            send_ref[...] = first


def gram_halves(matrix, row_count, bit):
    rows, width = matrix.shape
    tile = min(rows, 512)
    half = jax.ShapeDtypeStruct((STACK, BLOCK), jnp.float32)
    return pl.pallas_call(
        functools.partial(gram_kernel, row_count),
        out_shape=(half, half),
        grid=(rows // tile,),
        in_specs=[
            pl.BlockSpec(memory_space=pltpu.SMEM),
            pl.BlockSpec((tile, width), lambda i: (i, 0)),
        ],
        out_specs=(
            pl.BlockSpec((STACK, BLOCK), lambda i: (0, 0)),
            pl.BlockSpec((STACK, BLOCK), lambda i: (0, 0)),
        ),
        scratch_shapes=[pltpu.VMEM((width, width), jnp.float32)],
    )(bit, matrix)


def group_index(axis, shift, size):
    return (lax.axis_index(axis) >> shift) & (size - 1)


def partner_xor(value, axis, shift, offset):
    mask = offset << shift
    pairs = [(source, source ^ mask) for source in range(lax.axis_size(axis))]
    return lax.ppermute(value, axis, pairs)


def scatter_sum(value, axis, shift, size):
    height = value.shape[0] // size
    index = group_index(axis, shift, size)
    chunk = lambda j: lax.dynamic_slice_in_dim(value, j * height, height, 0)
    total = chunk(index)
    for offset in range(1, size):
        total = total + partner_xor(chunk(index ^ offset), axis, shift, offset)
    return total


def gather_all(chunk, axis, shift, size):
    height = chunk.shape[0]
    index = group_index(axis, shift, size)
    whole = jnp.zeros((height * size, chunk.shape[1]), chunk.dtype)
    whole = lax.dynamic_update_slice_in_dim(whole, chunk, index * height, 0)
    for offset in range(1, size):
        got = partner_xor(chunk, axis, shift, offset)
        whole = lax.dynamic_update_slice_in_dim(whole, got, (index ^ offset) * height, 0)
    return whole


def axis_groups(axis, first):
    bits = lax.axis_size(axis).bit_length() - 1
    groups = []
    shift = first
    while shift < bits:
        width = min(2, bits - shift)
        groups.append((axis, shift, 2**width))
        shift += width
    return groups


def group_total(value, axis, shift, size):
    index = group_index(axis, shift, size)
    received = [value] + [partner_xor(value, axis, shift, offset) for offset in range(1, size)]
    ordered = []
    for slot in range(size):
        pick = received[0]
        for offset in range(1, size):
            pick = jnp.where((index ^ offset) == slot, received[offset], pick)
        ordered.append(pick)
    return functools.reduce(jnp.add, ordered)


def on_device(response):
    row_count = response.shape[0] * lax.axis_size("inner") * lax.axis_size("wide")
    bit = jnp.reshape(lax.axis_index("wide") & 1, (1,)).astype(jnp.int32)
    keep, send = gram_halves(response, row_count, bit)
    partial_sum = keep + partner_xor(send, "wide", 0, 1)
    groups = axis_groups("inner", 0) + axis_groups("wide", 1)
    for group in groups[:-1]:
        partial_sum = scatter_sum(partial_sum, *group)
    partial_sum = group_total(partial_sum, *groups[-1])
    for group in reversed(groups[:-1]):
        partial_sum = gather_all(partial_sum, *group)
    got = partner_xor(partial_sum, "wide", 0, 1)
    upper_factor, inverse_upper = cholesky_and_inverse(bit, partial_sum, got)
    q_rows = rows_times(response, inverse_upper)
    return (upper_factor, q_rows)


def solution(mesh):
    in_specs = (P(("inner", "wide"), None),)
    out_specs = (P(), P(("inner", "wide"), None))
    return jax.shard_map(
        on_device, mesh=mesh, in_specs=in_specs, out_specs=out_specs, check_vma=False
    )
```

```python
import functools

import jax
import jax.numpy as jnp
from jax import lax
from jax.experimental import pallas as pl
from jax.experimental.pallas import tpu as pltpu
from jax.sharding import PartitionSpec as P


BLOCK = 128
SLAB = 8


STACK = 5 * BLOCK


def fill_gram(work_ref, first_ref, second_ref):
    b = BLOCK
    work_ref[:, 0:b] = first_ref[0:4 * b, :]
    work_ref[b:2 * b, b:2 * b] = first_ref[4 * b:5 * b, :]
    work_ref[2 * b:4 * b, b:2 * b] = second_ref[0:2 * b, :]
    work_ref[2 * b:4 * b, 2 * b:3 * b] = second_ref[2 * b:4 * b, :]
    work_ref[3 * b:4 * b, 3 * b:4 * b] = second_ref[4 * b:5 * b, :]
    for i in range(4):
        for j in range(i + 1, 4):
            work_ref[i * b:(i + 1) * b, j * b:(j + 1) * b] = work_ref[j * b:(j + 1) * b, i * b:(i + 1) * b].T


def hdot(left, right):
    return jnp.dot(left, right, precision=lax.Precision.HIGHEST, preferred_element_type=jnp.float32)


def sweep_block(diag):
    size = diag.shape[0]
    eye = (lax.broadcasted_iota(jnp.int32, (size, size), 0) == lax.broadcasted_iota(jnp.int32, (size, size), 1)).astype(jnp.float32)
    joined = jnp.concatenate([diag, eye], axis=1)
    slabs = [joined[s * SLAB:(s + 1) * SLAB] for s in range(size // SLAB)]
    rows = lax.broadcasted_iota(jnp.int32, (SLAB, 1), 0)
    for j in range(size):
        s, t = divmod(j, SLAB)
        scale = lax.rsqrt(slabs[s][t:t + 1, j:j + 1])
        top = slabs[s][t:t + 1, :] * scale
        for q in range(s + 1, len(slabs)):
            slabs[q] = slabs[q] - (slabs[q][:, j:j + 1] * scale) * top
        here = slabs[s]
        updated = here - (here[:, j:j + 1] * scale) * top
        slabs[s] = jnp.where(rows > t, updated, jnp.where(rows == t, top, here))
    joined = jnp.concatenate(slabs, axis=0)
    r = lax.broadcasted_iota(jnp.int32, (size, size), 0)
    c = lax.broadcasted_iota(jnp.int32, (size, size), 1)
    return jnp.where(c >= r, joined[:, :size], 0.0), joined[:, size:]


def chol_kernel(bit_ref, mine_ref, got_ref, u_ref, uinv_ref, work_ref, aug_ref, inv_ref):
    n = u_ref.shape[0]

    @pl.when(bit_ref[0] == 0)
    def _():
        fill_gram(work_ref, mine_ref, got_ref)

    @pl.when(bit_ref[0] != 0)
    def _():
        fill_gram(work_ref, got_ref, mine_ref)

    aug_ref[...] = jnp.zeros_like(aug_ref)
    blocks = n // BLOCK
    for k in range(blocks):
        lo, hi = k * BLOCK, (k + 1) * BLOCK
        if hi < n:
            u_ref[hi:n, lo:hi] = jnp.zeros((n - hi, BLOCK), jnp.float32)
            uinv_ref[hi:n, lo:hi] = jnp.zeros((n - hi, BLOCK), jnp.float32)
        u_kk, inv_kk = sweep_block(work_ref[lo:hi, lo:hi])
        u_ref[lo:hi, lo:hi] = u_kk
        if k > 0:
            inv_row = hdot(inv_kk, aug_ref[lo:hi, 0:lo])
            inv_ref[lo:hi, 0:lo] = inv_row
            uinv_ref[0:lo, lo:hi] = inv_row.T
        inv_ref[lo:hi, lo:hi] = inv_kk
        uinv_ref[lo:hi, lo:hi] = inv_kk.T
        if hi < n:
            u_off = hdot(inv_kk, work_ref[lo:hi, hi:n])
            u_ref[lo:hi, hi:n] = u_off
            u_off_t = u_off.T
            work_ref[hi:n, hi:n] = work_ref[hi:n, hi:n] - hdot(u_off_t, u_off)
            aug_ref[hi:n, 0:hi] = aug_ref[hi:n, 0:hi] - hdot(u_off_t, inv_ref[lo:hi, 0:hi])


def cholesky_and_inverse(bit, mine, got):
    n = 4 * BLOCK
    spec = pl.BlockSpec(memory_space=pltpu.VMEM)
    return pl.pallas_call(
        chol_kernel,
        out_shape=(jax.ShapeDtypeStruct((n, n), jnp.float32), jax.ShapeDtypeStruct((n, n), jnp.float32)),
        in_specs=[pl.BlockSpec(memory_space=pltpu.SMEM), spec, spec],
        out_specs=(spec, spec),
        scratch_shapes=[pltpu.VMEM((n, n), jnp.float32) for _ in range(3)],
    )(bit, mine, got)


def rows_kernel(a_ref, w_ref, o_ref):
    width = w_ref.shape[1]
    half = width // 2
    o_ref[:, 0:half] = hdot(a_ref[:, 0:half], w_ref[0:half, 0:half])
    o_ref[:, half:width] = hdot(a_ref[...], w_ref[:, half:width])


def rows_times(matrix, weights):
    rows, width = matrix.shape
    tile = min(rows, 512)
    return pl.pallas_call(
        rows_kernel,
        out_shape=jax.ShapeDtypeStruct((rows, weights.shape[1]), jnp.float32),
        grid=(rows // tile,),
        in_specs=[
            pl.BlockSpec((tile, width), lambda i: (i, 0)),
            pl.BlockSpec(weights.shape, lambda i: (0, 0)),
        ],
        out_specs=pl.BlockSpec((tile, weights.shape[1]), lambda i: (i, 0)),
    )(matrix, weights)


def matmul(left, right):
    return jnp.dot(left, right, precision=lax.Precision.HIGHEST, preferred_element_type=jnp.float32)


def cross(left, right):
    return lax.dot_general(
        left,
        right,
        (((0,), (0,)), ((), ())),
        precision=lax.Precision.HIGHEST,
        preferred_element_type=jnp.float32,
    )


def stack_blocks(a, which):
    b = BLOCK
    if which == 0:
        return [cross(a, a[:, 0:b]), cross(a[:, b:2 * b], a[:, b:2 * b])]
    return [
        cross(a[:, 2 * b:4 * b], a[:, b:2 * b]),
        cross(a[:, 2 * b:4 * b], a[:, 2 * b:3 * b]),
        cross(a[:, 3 * b:4 * b], a[:, 3 * b:4 * b]),
    ]


def stack_kernel(row_count, flip, bit_ref, a_ref, o_ref):
    step = pl.program_id(0)

    @pl.when(step == 0)
    def _():
        o_ref[...] = jnp.zeros_like(o_ref)

    a = a_ref[...]
    for which in (0, 1):

        @pl.when((bit_ref[0] ^ flip) == which)
        def _():
            start = 0
            for block in stack_blocks(a, which):
                o_ref[start:start + block.shape[0], :] += block
                start += block.shape[0]

    @pl.when(step == pl.num_programs(0) - 1)
    def _():
        o_ref[...] = o_ref[...] / row_count


def gram_stack(matrix, row_count, bit, flip):
    rows, width = matrix.shape
    tile = min(rows, 512)
    return pl.pallas_call(
        functools.partial(stack_kernel, row_count, flip),
        out_shape=jax.ShapeDtypeStruct((STACK, BLOCK), jnp.float32),
        grid=(rows // tile,),
        in_specs=[
            pl.BlockSpec(memory_space=pltpu.SMEM),
            pl.BlockSpec((tile, width), lambda i: (i, 0)),
        ],
        out_specs=pl.BlockSpec((STACK, BLOCK), lambda i: (0, 0)),
    )(bit, matrix)


def group_index(axis, shift, size):
    return (lax.axis_index(axis) >> shift) & (size - 1)


def partner_xor(value, axis, shift, offset):
    mask = offset << shift
    pairs = [(source, source ^ mask) for source in range(lax.axis_size(axis))]
    return lax.ppermute(value, axis, pairs)


def scatter_sum(value, axis, shift, size):
    height = value.shape[0] // size
    index = group_index(axis, shift, size)
    chunk = lambda j: lax.dynamic_slice_in_dim(value, j * height, height, 0)
    total = chunk(index)
    for offset in range(1, size):
        total = total + partner_xor(chunk(index ^ offset), axis, shift, offset)
    return total


def gather_all(chunk, axis, shift, size):
    height = chunk.shape[0]
    index = group_index(axis, shift, size)
    whole = jnp.zeros((height * size, chunk.shape[1]), chunk.dtype)
    whole = lax.dynamic_update_slice_in_dim(whole, chunk, index * height, 0)
    for offset in range(1, size):
        got = partner_xor(chunk, axis, shift, offset)
        whole = lax.dynamic_update_slice_in_dim(whole, got, (index ^ offset) * height, 0)
    return whole


def axis_groups(axis, first):
    bits = lax.axis_size(axis).bit_length() - 1
    groups = []
    shift = first
    while shift < bits:
        width = min(2, bits - shift)
        groups.append((axis, shift, 2**width))
        shift += width
    return groups


def group_total(value, axis, shift, size):
    index = group_index(axis, shift, size)
    received = [value] + [partner_xor(value, axis, shift, offset) for offset in range(1, size)]
    ordered = []
    for slot in range(size):
        pick = received[0]
        for offset in range(1, size):
            pick = jnp.where((index ^ offset) == slot, received[offset], pick)
        ordered.append(pick)
    return functools.reduce(jnp.add, ordered)


def on_device(response):
    row_count = response.shape[0] * lax.axis_size("inner") * lax.axis_size("wide")
    bit = jnp.reshape(lax.axis_index("wide") & 1, (1,)).astype(jnp.int32)
    send = gram_stack(response, row_count, bit, 1)
    received = partner_xor(send, "wide", 0, 1)
    keep = gram_stack(response, row_count, bit, 0)
    partial_sum = keep + received
    groups = axis_groups("inner", 0) + axis_groups("wide", 1)
    for group in groups[:-1]:
        partial_sum = scatter_sum(partial_sum, *group)
    partial_sum = group_total(partial_sum, *groups[-1])
    for group in reversed(groups[:-1]):
        partial_sum = gather_all(partial_sum, *group)
    got = partner_xor(partial_sum, "wide", 0, 1)
    upper_factor, inverse_upper = cholesky_and_inverse(bit, partial_sum, got)
    q_rows = rows_times(response, inverse_upper)
    return (upper_factor, q_rows)


def solution(mesh):
    in_specs = (P(("inner", "wide"), None),)
    out_specs = (P(), P(("inner", "wide"), None))
    return jax.shard_map(
        on_device, mesh=mesh, in_specs=in_specs, out_specs=out_specs, check_vma=False
    )
```

```python
import functools

import jax
import jax.numpy as jnp
from jax import lax
from jax.experimental import pallas as pl
from jax.experimental.pallas import tpu as pltpu
from jax.sharding import PartitionSpec as P


BLOCK = 128
SLAB = 8


STACK = 5 * BLOCK


def lower_stacks(acc_ref):
    b = BLOCK
    first = jnp.concatenate([acc_ref[:, 0:b], acc_ref[b:2 * b, b:2 * b]], axis=0)
    second = jnp.concatenate(
        [acc_ref[2 * b:4 * b, b:2 * b], acc_ref[2 * b:4 * b, 2 * b:3 * b], acc_ref[3 * b:4 * b, 3 * b:4 * b]], axis=0
    )
    return first, second


def fill_gram(work_ref, first_ref, second_ref):
    b = BLOCK
    work_ref[:, 0:b] = first_ref[0:4 * b, :]
    work_ref[b:2 * b, b:2 * b] = first_ref[4 * b:5 * b, :]
    work_ref[2 * b:4 * b, b:2 * b] = second_ref[0:2 * b, :]
    work_ref[2 * b:4 * b, 2 * b:3 * b] = second_ref[2 * b:4 * b, :]
    work_ref[3 * b:4 * b, 3 * b:4 * b] = second_ref[4 * b:5 * b, :]
    for i in range(4):
        for j in range(i + 1, 4):
            work_ref[i * b:(i + 1) * b, j * b:(j + 1) * b] = work_ref[j * b:(j + 1) * b, i * b:(i + 1) * b].T


def hdot(left, right):
    return jnp.dot(left, right, precision=lax.Precision.HIGHEST, preferred_element_type=jnp.float32)


def sweep_block(diag):
    size = diag.shape[0]
    eye = (lax.broadcasted_iota(jnp.int32, (size, size), 0) == lax.broadcasted_iota(jnp.int32, (size, size), 1)).astype(jnp.float32)
    joined = jnp.concatenate([diag, eye], axis=1)
    slabs = [joined[s * SLAB:(s + 1) * SLAB] for s in range(size // SLAB)]
    rows = lax.broadcasted_iota(jnp.int32, (SLAB, 1), 0)
    for j in range(size):
        s, t = divmod(j, SLAB)
        scale = lax.rsqrt(slabs[s][t:t + 1, j:j + 1])
        top = slabs[s][t:t + 1, :] * scale
        for q in range(s + 1, len(slabs)):
            slabs[q] = slabs[q] - (slabs[q][:, j:j + 1] * scale) * top
        here = slabs[s]
        updated = here - (here[:, j:j + 1] * scale) * top
        slabs[s] = jnp.where(rows > t, updated, jnp.where(rows == t, top, here))
    joined = jnp.concatenate(slabs, axis=0)
    r = lax.broadcasted_iota(jnp.int32, (size, size), 0)
    c = lax.broadcasted_iota(jnp.int32, (size, size), 1)
    return jnp.where(c >= r, joined[:, :size], 0.0), joined[:, size:]


def chol_kernel(bit_ref, mine_ref, got_ref, u_ref, uinv_ref, work_ref, aug_ref, inv_ref):
    n = u_ref.shape[0]

    @pl.when(bit_ref[0] == 0)
    def _():
        fill_gram(work_ref, mine_ref, got_ref)

    @pl.when(bit_ref[0] != 0)
    def _():
        fill_gram(work_ref, got_ref, mine_ref)

    aug_ref[...] = jnp.zeros_like(aug_ref)
    blocks = n // BLOCK
    for k in range(blocks):
        lo, hi = k * BLOCK, (k + 1) * BLOCK
        if hi < n:
            u_ref[hi:n, lo:hi] = jnp.zeros((n - hi, BLOCK), jnp.float32)
            uinv_ref[hi:n, lo:hi] = jnp.zeros((n - hi, BLOCK), jnp.float32)
        u_kk, inv_kk = sweep_block(work_ref[lo:hi, lo:hi])
        u_ref[lo:hi, lo:hi] = u_kk
        if k > 0:
            inv_row = hdot(inv_kk, aug_ref[lo:hi, 0:lo])
            inv_ref[lo:hi, 0:lo] = inv_row
            uinv_ref[0:lo, lo:hi] = inv_row.T
        inv_ref[lo:hi, lo:hi] = inv_kk
        uinv_ref[lo:hi, lo:hi] = inv_kk.T
        if hi < n:
            u_off = hdot(inv_kk, work_ref[lo:hi, hi:n])
            u_ref[lo:hi, hi:n] = u_off
            u_off_t = u_off.T
            work_ref[hi:n, hi:n] = work_ref[hi:n, hi:n] - hdot(u_off_t, u_off)
            aug_ref[hi:n, 0:hi] = aug_ref[hi:n, 0:hi] - hdot(u_off_t, inv_ref[lo:hi, 0:hi])


def cholesky_and_inverse(bit, mine, got):
    n = 4 * BLOCK
    spec = pl.BlockSpec(memory_space=pltpu.VMEM)
    return pl.pallas_call(
        chol_kernel,
        out_shape=(jax.ShapeDtypeStruct((n, n), jnp.float32), jax.ShapeDtypeStruct((n, n), jnp.float32)),
        in_specs=[pl.BlockSpec(memory_space=pltpu.SMEM), spec, spec],
        out_specs=(spec, spec),
        scratch_shapes=[pltpu.VMEM((n, n), jnp.float32) for _ in range(3)],
    )(bit, mine, got)


def rows_kernel(a_ref, w_ref, o_ref):
    width = w_ref.shape[1]
    half = width // 2
    o_ref[:, 0:half] = hdot(a_ref[:, 0:half], w_ref[0:half, 0:half])
    o_ref[:, half:width] = hdot(a_ref[...], w_ref[:, half:width])


def rows_times(matrix, weights):
    rows, width = matrix.shape
    tile = min(rows, 512)
    return pl.pallas_call(
        rows_kernel,
        out_shape=jax.ShapeDtypeStruct((rows, weights.shape[1]), jnp.float32),
        grid=(rows // tile,),
        in_specs=[
            pl.BlockSpec((tile, width), lambda i: (i, 0)),
            pl.BlockSpec(weights.shape, lambda i: (0, 0)),
        ],
        out_specs=pl.BlockSpec((tile, weights.shape[1]), lambda i: (i, 0)),
    )(matrix, weights)


def matmul(left, right):
    return jnp.dot(left, right, precision=lax.Precision.HIGHEST, preferred_element_type=jnp.float32)


def cross(left, right):
    return lax.dot_general(
        left,
        right,
        (((0,), (0,)), ((), ())),
        precision=lax.Precision.HIGHEST,
        preferred_element_type=jnp.float32,
    )


def gram_kernel(row_count, bit_ref, a_ref, keep_ref, send_ref, acc_ref):
    step = pl.program_id(0)
    half = a_ref.shape[1] // 2

    @pl.when(step == 0)
    def _():
        acc_ref[...] = jnp.zeros_like(acc_ref)

    a = a_ref[...]
    acc_ref[:, 0:half] += cross(a, a[:, 0:half])
    acc_ref[half:, half:] += cross(a[:, half:], a[:, half:])

    @pl.when(step == pl.num_programs(0) - 1)
    def _():
        first, second = lower_stacks(acc_ref)
        first = first / row_count
        second = second / row_count

        @pl.when(bit_ref[0] == 0)
        def _():
            keep_ref[...] = first
            send_ref[...] = second

        @pl.when(bit_ref[0] != 0)
        def _():
            keep_ref[...] = second
            send_ref[...] = first


def gram_halves(matrix, row_count, bit):
    rows, width = matrix.shape
    tile = min(rows, 512)
    half = jax.ShapeDtypeStruct((STACK, BLOCK), jnp.float32)
    return pl.pallas_call(
        functools.partial(gram_kernel, row_count),
        out_shape=(half, half),
        grid=(rows // tile,),
        in_specs=[
            pl.BlockSpec(memory_space=pltpu.SMEM),
            pl.BlockSpec((tile, width), lambda i: (i, 0)),
        ],
        out_specs=(
            pl.BlockSpec((STACK, BLOCK), lambda i: (0, 0)),
            pl.BlockSpec((STACK, BLOCK), lambda i: (0, 0)),
        ),
        scratch_shapes=[pltpu.VMEM((width, width), jnp.float32)],
    )(bit, matrix)


def group_index(axis, shift, size):
    return (lax.axis_index(axis) >> shift) & (size - 1)


def partner_xor(value, axis, shift, offset):
    mask = offset << shift
    pairs = [(source, source ^ mask) for source in range(lax.axis_size(axis))]
    return lax.ppermute(value, axis, pairs)


def scatter_sum(value, axis, shift, size):
    height = value.shape[0] // size
    index = group_index(axis, shift, size)
    chunk = lambda j: lax.dynamic_slice_in_dim(value, j * height, height, 0)
    total = chunk(index)
    for offset in range(1, size):
        total = total + partner_xor(chunk(index ^ offset), axis, shift, offset)
    return total


def gather_all(chunk, axis, shift, size):
    height = chunk.shape[0]
    index = group_index(axis, shift, size)
    whole = jnp.zeros((height * size, chunk.shape[1]), chunk.dtype)
    whole = lax.dynamic_update_slice_in_dim(whole, chunk, index * height, 0)
    for offset in range(1, size):
        got = partner_xor(chunk, axis, shift, offset)
        whole = lax.dynamic_update_slice_in_dim(whole, got, (index ^ offset) * height, 0)
    return whole


def axis_groups(axis, first):
    bits = lax.axis_size(axis).bit_length() - 1
    groups = []
    shift = first
    while shift < bits:
        width = min(2, bits - shift)
        groups.append((axis, shift, 2**width))
        shift += width
    return groups


def group_total(value, axis, shift, size):
    index = group_index(axis, shift, size)
    received = [value] + [partner_xor(value, axis, shift, offset) for offset in range(1, size)]
    ordered = []
    for slot in range(size):
        pick = received[0]
        for offset in range(1, size):
            pick = jnp.where((index ^ offset) == slot, received[offset], pick)
        ordered.append(pick)
    return functools.reduce(jnp.add, ordered)


def on_device(response):
    row_count = response.shape[0] * lax.axis_size("inner") * lax.axis_size("wide")
    bit = jnp.reshape(lax.axis_index("wide") & 1, (1,)).astype(jnp.int32)
    keep, send = gram_halves(response, row_count, bit)
    partial_sum = keep + partner_xor(send, "wide", 0, 1)
    groups = axis_groups("wide", 1) + axis_groups("inner", 0)
    for group in groups[:-1]:
        partial_sum = scatter_sum(partial_sum, *group)
    partial_sum = group_total(partial_sum, *groups[-1])
    for group in reversed(groups[:-1]):
        partial_sum = gather_all(partial_sum, *group)
    got = partner_xor(partial_sum, "wide", 0, 1)
    upper_factor, inverse_upper = cholesky_and_inverse(bit, partial_sum, got)
    q_rows = rows_times(response, inverse_upper)
    return (upper_factor, q_rows)


def solution(mesh):
    in_specs = (P(("inner", "wide"), None),)
    out_specs = (P(), P(("inner", "wide"), None))
    return jax.shard_map(
        on_device, mesh=mesh, in_specs=in_specs, out_specs=out_specs, check_vma=False
    )
```

```python
import functools

import jax
import jax.numpy as jnp
from jax import lax
from jax.experimental import pallas as pl
from jax.experimental.pallas import tpu as pltpu
from jax.sharding import PartitionSpec as P


BLOCK = 128
SLAB = 8


PAD = 32
STACK = 4 * BLOCK + PAD


def local_grid(size):
    return lax.broadcasted_iota(jnp.int32, (size, size), 0), lax.broadcasted_iota(jnp.int32, (size, size), 1)


def pack_pair(first, second):
    r, c = local_grid(first.shape[0])
    packed = jnp.where(r > c, first, second)
    diagonal = jnp.sum(jnp.where(r == c, first, 0.0), axis=0, keepdims=True)
    pad = jnp.concatenate([diagonal, jnp.zeros((PAD - 1, first.shape[0]), jnp.float32)], axis=0)
    return packed, pad


def unpack_pair(packed, diagonal):
    r, c = local_grid(packed.shape[0])
    flipped = packed.T
    first = jnp.where(r > c, packed, jnp.where(r == c, diagonal, flipped))
    second = jnp.where(r <= c, packed, flipped)
    return first, second


def lower_stacks(acc_ref):
    b = BLOCK
    p01, d0 = pack_pair(acc_ref[0:b, 0:b], acc_ref[b:2 * b, b:2 * b])
    p23, d2 = pack_pair(acc_ref[2 * b:3 * b, 2 * b:3 * b], acc_ref[3 * b:4 * b, 3 * b:4 * b])
    first = jnp.concatenate([acc_ref[b:4 * b, 0:b], p01, d0], axis=0)
    second = jnp.concatenate([acc_ref[2 * b:4 * b, b:2 * b], acc_ref[3 * b:4 * b, 2 * b:3 * b], p23, d2], axis=0)
    return first, second


def fill_gram(work_ref, first_ref, second_ref):
    b = BLOCK
    work_ref[b:4 * b, 0:b] = first_ref[0:3 * b, :]
    d0, d1 = unpack_pair(first_ref[3 * b:4 * b, :], first_ref[4 * b:4 * b + 1, :])
    work_ref[0:b, 0:b] = d0
    work_ref[b:2 * b, b:2 * b] = d1
    work_ref[2 * b:4 * b, b:2 * b] = second_ref[0:2 * b, :]
    work_ref[3 * b:4 * b, 2 * b:3 * b] = second_ref[2 * b:3 * b, :]
    d2, d3 = unpack_pair(second_ref[3 * b:4 * b, :], second_ref[4 * b:4 * b + 1, :])
    work_ref[2 * b:3 * b, 2 * b:3 * b] = d2
    work_ref[3 * b:4 * b, 3 * b:4 * b] = d3
    for i in range(4):
        for j in range(i + 1, 4):
            work_ref[i * b:(i + 1) * b, j * b:(j + 1) * b] = work_ref[j * b:(j + 1) * b, i * b:(i + 1) * b].T


def hdot(left, right):
    return jnp.dot(left, right, precision=lax.Precision.HIGHEST, preferred_element_type=jnp.float32)


def sweep_block(diag):
    size = diag.shape[0]
    eye = (lax.broadcasted_iota(jnp.int32, (size, size), 0) == lax.broadcasted_iota(jnp.int32, (size, size), 1)).astype(jnp.float32)
    joined = jnp.concatenate([diag, eye], axis=1)
    slabs = [joined[s * SLAB:(s + 1) * SLAB] for s in range(size // SLAB)]
    rows = lax.broadcasted_iota(jnp.int32, (SLAB, 1), 0)
    for j in range(size):
        s, t = divmod(j, SLAB)
        scale = lax.rsqrt(slabs[s][t:t + 1, j:j + 1])
        top = slabs[s][t:t + 1, :] * scale
        for q in range(s + 1, len(slabs)):
            slabs[q] = slabs[q] - (slabs[q][:, j:j + 1] * scale) * top
        here = slabs[s]
        updated = here - (here[:, j:j + 1] * scale) * top
        slabs[s] = jnp.where(rows > t, updated, jnp.where(rows == t, top, here))
    joined = jnp.concatenate(slabs, axis=0)
    r = lax.broadcasted_iota(jnp.int32, (size, size), 0)
    c = lax.broadcasted_iota(jnp.int32, (size, size), 1)
    return jnp.where(c >= r, joined[:, :size], 0.0), joined[:, size:]


def chol_kernel(bit_ref, mine_ref, got_ref, u_ref, uinv_ref, work_ref, aug_ref, inv_ref):
    n = u_ref.shape[0]

    @pl.when(bit_ref[0] == 0)
    def _():
        fill_gram(work_ref, mine_ref, got_ref)

    @pl.when(bit_ref[0] != 0)
    def _():
        fill_gram(work_ref, got_ref, mine_ref)

    aug_ref[...] = jnp.zeros_like(aug_ref)
    blocks = n // BLOCK
    for k in range(blocks):
        lo, hi = k * BLOCK, (k + 1) * BLOCK
        if hi < n:
            u_ref[hi:n, lo:hi] = jnp.zeros((n - hi, BLOCK), jnp.float32)
            uinv_ref[hi:n, lo:hi] = jnp.zeros((n - hi, BLOCK), jnp.float32)
        u_kk, inv_kk = sweep_block(work_ref[lo:hi, lo:hi])
        u_ref[lo:hi, lo:hi] = u_kk
        if k > 0:
            inv_row = hdot(inv_kk, aug_ref[lo:hi, 0:lo])
            inv_ref[lo:hi, 0:lo] = inv_row
            uinv_ref[0:lo, lo:hi] = inv_row.T
        inv_ref[lo:hi, lo:hi] = inv_kk
        uinv_ref[lo:hi, lo:hi] = inv_kk.T
        if hi < n:
            u_off = hdot(inv_kk, work_ref[lo:hi, hi:n])
            u_ref[lo:hi, hi:n] = u_off
            u_off_t = u_off.T
            work_ref[hi:n, hi:n] = work_ref[hi:n, hi:n] - hdot(u_off_t, u_off)
            aug_ref[hi:n, 0:hi] = aug_ref[hi:n, 0:hi] - hdot(u_off_t, inv_ref[lo:hi, 0:hi])


def cholesky_and_inverse(bit, mine, got):
    n = 4 * BLOCK
    spec = pl.BlockSpec(memory_space=pltpu.VMEM)
    return pl.pallas_call(
        chol_kernel,
        out_shape=(jax.ShapeDtypeStruct((n, n), jnp.float32), jax.ShapeDtypeStruct((n, n), jnp.float32)),
        in_specs=[pl.BlockSpec(memory_space=pltpu.SMEM), spec, spec],
        out_specs=(spec, spec),
        scratch_shapes=[pltpu.VMEM((n, n), jnp.float32) for _ in range(3)],
    )(bit, mine, got)


def rows_kernel(a_ref, w_ref, o_ref):
    width = w_ref.shape[1]
    half = width // 2
    o_ref[:, 0:half] = hdot(a_ref[:, 0:half], w_ref[0:half, 0:half])
    o_ref[:, half:width] = hdot(a_ref[...], w_ref[:, half:width])


def rows_times(matrix, weights):
    rows, width = matrix.shape
    tile = min(rows, 512)
    return pl.pallas_call(
        rows_kernel,
        out_shape=jax.ShapeDtypeStruct((rows, weights.shape[1]), jnp.float32),
        grid=(rows // tile,),
        in_specs=[
            pl.BlockSpec((tile, width), lambda i: (i, 0)),
            pl.BlockSpec(weights.shape, lambda i: (0, 0)),
        ],
        out_specs=pl.BlockSpec((tile, weights.shape[1]), lambda i: (i, 0)),
    )(matrix, weights)


def matmul(left, right):
    return jnp.dot(left, right, precision=lax.Precision.HIGHEST, preferred_element_type=jnp.float32)


def cross(left, right):
    return lax.dot_general(
        left,
        right,
        (((0,), (0,)), ((), ())),
        precision=lax.Precision.HIGHEST,
        preferred_element_type=jnp.float32,
    )


def gram_kernel(row_count, bit_ref, a_ref, keep_ref, send_ref, acc_ref):
    step = pl.program_id(0)
    half = a_ref.shape[1] // 2

    @pl.when(step == 0)
    def _():
        acc_ref[...] = jnp.zeros_like(acc_ref)

    a = a_ref[...]
    acc_ref[:, 0:half] += cross(a, a[:, 0:half])
    acc_ref[half:, half:] += cross(a[:, half:], a[:, half:])

    @pl.when(step == pl.num_programs(0) - 1)
    def _():
        first, second = lower_stacks(acc_ref)
        first = first / row_count
        second = second / row_count

        @pl.when(bit_ref[0] == 0)
        def _():
            keep_ref[...] = first
            send_ref[...] = second

        @pl.when(bit_ref[0] != 0)
        def _():
            keep_ref[...] = second
            send_ref[...] = first


def gram_halves(matrix, row_count, bit):
    rows, width = matrix.shape
    tile = min(rows, 512)
    half = jax.ShapeDtypeStruct((STACK, BLOCK), jnp.float32)
    return pl.pallas_call(
        functools.partial(gram_kernel, row_count),
        out_shape=(half, half),
        grid=(rows // tile,),
        in_specs=[
            pl.BlockSpec(memory_space=pltpu.SMEM),
            pl.BlockSpec((tile, width), lambda i: (i, 0)),
        ],
        out_specs=(
            pl.BlockSpec((STACK, BLOCK), lambda i: (0, 0)),
            pl.BlockSpec((STACK, BLOCK), lambda i: (0, 0)),
        ),
        scratch_shapes=[pltpu.VMEM((width, width), jnp.float32)],
    )(bit, matrix)


def group_index(axis, shift, size):
    return (lax.axis_index(axis) >> shift) & (size - 1)


def partner_xor(value, axis, shift, offset):
    mask = offset << shift
    pairs = [(source, source ^ mask) for source in range(lax.axis_size(axis))]
    return lax.ppermute(value, axis, pairs)


def scatter_sum(value, axis, shift, size):
    height = value.shape[0] // size
    index = group_index(axis, shift, size)
    chunk = lambda j: lax.dynamic_slice_in_dim(value, j * height, height, 0)
    total = chunk(index)
    for offset in range(1, size):
        total = total + partner_xor(chunk(index ^ offset), axis, shift, offset)
    return total


def gather_all(chunk, axis, shift, size):
    height = chunk.shape[0]
    index = group_index(axis, shift, size)
    whole = jnp.zeros((height * size, chunk.shape[1]), chunk.dtype)
    whole = lax.dynamic_update_slice_in_dim(whole, chunk, index * height, 0)
    for offset in range(1, size):
        got = partner_xor(chunk, axis, shift, offset)
        whole = lax.dynamic_update_slice_in_dim(whole, got, (index ^ offset) * height, 0)
    return whole


def axis_groups(axis, first):
    bits = lax.axis_size(axis).bit_length() - 1
    groups = []
    shift = first
    while shift < bits:
        width = min(2, bits - shift)
        groups.append((axis, shift, 2**width))
        shift += width
    return groups


def group_total(value, axis, shift, size):
    index = group_index(axis, shift, size)
    received = [value] + [partner_xor(value, axis, shift, offset) for offset in range(1, size)]
    ordered = []
    for slot in range(size):
        pick = received[0]
        for offset in range(1, size):
            pick = jnp.where((index ^ offset) == slot, received[offset], pick)
        ordered.append(pick)
    return functools.reduce(jnp.add, ordered)


def on_device(response):
    row_count = response.shape[0] * lax.axis_size("inner") * lax.axis_size("wide")
    bit = jnp.reshape(lax.axis_index("wide") & 1, (1,)).astype(jnp.int32)
    keep, send = gram_halves(response, row_count, bit)
    partial_sum = keep + partner_xor(send, "wide", 0, 1)
    groups = axis_groups("inner", 0) + axis_groups("wide", 1)
    for group in groups[:-1]:
        partial_sum = scatter_sum(partial_sum, *group)
    partial_sum = group_total(partial_sum, *groups[-1])
    for group in reversed(groups[:-1]):
        partial_sum = gather_all(partial_sum, *group)
    got = partner_xor(partial_sum, "wide", 0, 1)
    upper_factor, inverse_upper = cholesky_and_inverse(bit, partial_sum, got)
    q_rows = rows_times(response, inverse_upper)
    return (upper_factor, q_rows)


def solution(mesh):
    in_specs = (P(("inner", "wide"), None),)
    out_specs = (P(), P(("inner", "wide"), None))
    return jax.shard_map(
        on_device, mesh=mesh, in_specs=in_specs, out_specs=out_specs, check_vma=False
    )
```

```python
import functools

import jax
import jax.numpy as jnp
from jax import lax
from jax.experimental import pallas as pl
from jax.experimental.pallas import tpu as pltpu
from jax.sharding import PartitionSpec as P


BLOCK = 128
SLAB = 8


PAD = 32
STACK = 4 * BLOCK + PAD


def local_grid(size):
    return lax.broadcasted_iota(jnp.int32, (size, size), 0), lax.broadcasted_iota(jnp.int32, (size, size), 1)


def pack_pair(first, second):
    r, c = local_grid(first.shape[0])
    packed = jnp.where(r > c, first, second)
    diagonal = jnp.sum(jnp.where(r == c, first, 0.0), axis=0, keepdims=True)
    pad = jnp.concatenate([diagonal, jnp.zeros((PAD - 1, first.shape[0]), jnp.float32)], axis=0)
    return packed, pad


def unpack_pair(packed, diagonal):
    r, c = local_grid(packed.shape[0])
    flipped = packed.T
    first = jnp.where(r > c, packed, jnp.where(r == c, diagonal, flipped))
    second = jnp.where(r <= c, packed, flipped)
    return first, second


def lower_stacks(acc_ref):
    b = BLOCK
    p01, d0 = pack_pair(acc_ref[0:b, 0:b], acc_ref[b:2 * b, b:2 * b])
    p23, d2 = pack_pair(acc_ref[2 * b:3 * b, 2 * b:3 * b], acc_ref[3 * b:4 * b, 3 * b:4 * b])
    first = jnp.concatenate([acc_ref[b:4 * b, 0:b], p01, d0], axis=0)
    second = jnp.concatenate([acc_ref[2 * b:4 * b, b:2 * b], acc_ref[3 * b:4 * b, 2 * b:3 * b], p23, d2], axis=0)
    return first, second


def fill_gram(work_ref, first_ref, second_ref):
    b = BLOCK
    work_ref[b:4 * b, 0:b] = first_ref[0:3 * b, :]
    d0, d1 = unpack_pair(first_ref[3 * b:4 * b, :], first_ref[4 * b:4 * b + 1, :])
    work_ref[0:b, 0:b] = d0
    work_ref[b:2 * b, b:2 * b] = d1
    work_ref[2 * b:4 * b, b:2 * b] = second_ref[0:2 * b, :]
    work_ref[3 * b:4 * b, 2 * b:3 * b] = second_ref[2 * b:3 * b, :]
    d2, d3 = unpack_pair(second_ref[3 * b:4 * b, :], second_ref[4 * b:4 * b + 1, :])
    work_ref[2 * b:3 * b, 2 * b:3 * b] = d2
    work_ref[3 * b:4 * b, 3 * b:4 * b] = d3
    for i in range(4):
        for j in range(i + 1, 4):
            work_ref[i * b:(i + 1) * b, j * b:(j + 1) * b] = work_ref[j * b:(j + 1) * b, i * b:(i + 1) * b].T


def hdot(left, right):
    return jnp.dot(left, right, precision=lax.Precision.HIGHEST, preferred_element_type=jnp.float32)


def sweep_block(diag):
    size = diag.shape[0]
    eye = (lax.broadcasted_iota(jnp.int32, (size, size), 0) == lax.broadcasted_iota(jnp.int32, (size, size), 1)).astype(jnp.float32)
    joined = jnp.concatenate([diag, eye], axis=1)
    slabs = [joined[s * SLAB:(s + 1) * SLAB] for s in range(size // SLAB)]
    rows = lax.broadcasted_iota(jnp.int32, (SLAB, 1), 0)
    for j in range(size):
        s, t = divmod(j, SLAB)
        scale = lax.rsqrt(slabs[s][t:t + 1, j:j + 1])
        top = slabs[s][t:t + 1, :] * scale
        for q in range(s + 1, len(slabs)):
            slabs[q] = slabs[q] - (slabs[q][:, j:j + 1] * scale) * top
        here = slabs[s]
        updated = here - (here[:, j:j + 1] * scale) * top
        slabs[s] = jnp.where(rows > t, updated, jnp.where(rows == t, top, here))
    joined = jnp.concatenate(slabs, axis=0)
    r = lax.broadcasted_iota(jnp.int32, (size, size), 0)
    c = lax.broadcasted_iota(jnp.int32, (size, size), 1)
    return jnp.where(c >= r, joined[:, :size], 0.0), joined[:, size:]


def chol_kernel(bit_ref, mine_ref, got_ref, u_ref, uinv_ref, work_ref, aug_ref, inv_ref):
    n = u_ref.shape[0]

    @pl.when(bit_ref[0] == 0)
    def _():
        fill_gram(work_ref, mine_ref, got_ref)

    @pl.when(bit_ref[0] != 0)
    def _():
        fill_gram(work_ref, got_ref, mine_ref)

    aug_ref[...] = jnp.zeros_like(aug_ref)
    blocks = n // BLOCK
    for k in range(blocks):
        lo, hi = k * BLOCK, (k + 1) * BLOCK
        if hi < n:
            u_ref[hi:n, lo:hi] = jnp.zeros((n - hi, BLOCK), jnp.float32)
            uinv_ref[hi:n, lo:hi] = jnp.zeros((n - hi, BLOCK), jnp.float32)
        u_kk, inv_kk = sweep_block(work_ref[lo:hi, lo:hi])
        u_ref[lo:hi, lo:hi] = u_kk
        if k > 0:
            inv_row = hdot(inv_kk, aug_ref[lo:hi, 0:lo])
            inv_ref[lo:hi, 0:lo] = inv_row
            uinv_ref[0:lo, lo:hi] = inv_row.T
        inv_ref[lo:hi, lo:hi] = inv_kk
        uinv_ref[lo:hi, lo:hi] = inv_kk.T
        if hi < n:
            u_off = hdot(inv_kk, work_ref[lo:hi, hi:n])
            u_ref[lo:hi, hi:n] = u_off
            u_off_t = u_off.T
            work_ref[hi:n, hi:n] = work_ref[hi:n, hi:n] - hdot(u_off_t, u_off)
            aug_ref[hi:n, 0:hi] = aug_ref[hi:n, 0:hi] - hdot(u_off_t, inv_ref[lo:hi, 0:hi])


def cholesky_and_inverse(bit, mine, got):
    n = 4 * BLOCK
    spec = pl.BlockSpec(memory_space=pltpu.VMEM)
    return pl.pallas_call(
        chol_kernel,
        out_shape=(jax.ShapeDtypeStruct((n, n), jnp.float32), jax.ShapeDtypeStruct((n, n), jnp.float32)),
        in_specs=[pl.BlockSpec(memory_space=pltpu.SMEM), spec, spec],
        out_specs=(spec, spec),
        scratch_shapes=[pltpu.VMEM((n, n), jnp.float32) for _ in range(3)],
    )(bit, mine, got)


def rows_kernel(a_ref, w_ref, o_ref):
    width = w_ref.shape[1]
    half = width // 2
    o_ref[:, 0:half] = hdot(a_ref[:, 0:half], w_ref[0:half, 0:half])
    o_ref[:, half:width] = hdot(a_ref[...], w_ref[:, half:width])


def rows_times(matrix, weights):
    rows, width = matrix.shape
    tile = min(rows, 1024)
    return pl.pallas_call(
        rows_kernel,
        out_shape=jax.ShapeDtypeStruct((rows, weights.shape[1]), jnp.float32),
        grid=(rows // tile,),
        in_specs=[
            pl.BlockSpec((tile, width), lambda i: (i, 0)),
            pl.BlockSpec(weights.shape, lambda i: (0, 0)),
        ],
        out_specs=pl.BlockSpec((tile, weights.shape[1]), lambda i: (i, 0)),
    )(matrix, weights)


def matmul(left, right):
    return jnp.dot(left, right, precision=lax.Precision.HIGHEST, preferred_element_type=jnp.float32)


def cross(left, right):
    return lax.dot_general(
        left,
        right,
        (((0,), (0,)), ((), ())),
        precision=lax.Precision.HIGHEST,
        preferred_element_type=jnp.float32,
    )


def gram_kernel(row_count, bit_ref, a_ref, keep_ref, send_ref, acc_ref):
    step = pl.program_id(0)
    half = a_ref.shape[1] // 2

    @pl.when(step == 0)
    def _():
        acc_ref[...] = jnp.zeros_like(acc_ref)

    a = a_ref[...]
    acc_ref[:, 0:half] += cross(a, a[:, 0:half])
    acc_ref[half:, half:] += cross(a[:, half:], a[:, half:])

    @pl.when(step == pl.num_programs(0) - 1)
    def _():
        first, second = lower_stacks(acc_ref)
        first = first / row_count
        second = second / row_count

        @pl.when(bit_ref[0] == 0)
        def _():
            keep_ref[...] = first
            send_ref[...] = second

        @pl.when(bit_ref[0] != 0)
        def _():
            keep_ref[...] = second
            send_ref[...] = first


def gram_halves(matrix, row_count, bit):
    rows, width = matrix.shape
    tile = min(rows, 512)
    half = jax.ShapeDtypeStruct((STACK, BLOCK), jnp.float32)
    return pl.pallas_call(
        functools.partial(gram_kernel, row_count),
        out_shape=(half, half),
        grid=(rows // tile,),
        in_specs=[
            pl.BlockSpec(memory_space=pltpu.SMEM),
            pl.BlockSpec((tile, width), lambda i: (i, 0)),
        ],
        out_specs=(
            pl.BlockSpec((STACK, BLOCK), lambda i: (0, 0)),
            pl.BlockSpec((STACK, BLOCK), lambda i: (0, 0)),
        ),
        scratch_shapes=[pltpu.VMEM((width, width), jnp.float32)],
    )(bit, matrix)


def group_index(axis, shift, size):
    return (lax.axis_index(axis) >> shift) & (size - 1)


def partner_xor(value, axis, shift, offset):
    mask = offset << shift
    pairs = [(source, source ^ mask) for source in range(lax.axis_size(axis))]
    return lax.ppermute(value, axis, pairs)


def scatter_sum(value, axis, shift, size):
    height = value.shape[0] // size
    index = group_index(axis, shift, size)
    chunk = lambda j: lax.dynamic_slice_in_dim(value, j * height, height, 0)
    total = chunk(index)
    for offset in range(1, size):
        total = total + partner_xor(chunk(index ^ offset), axis, shift, offset)
    return total


def gather_all(chunk, axis, shift, size):
    height = chunk.shape[0]
    index = group_index(axis, shift, size)
    whole = jnp.zeros((height * size, chunk.shape[1]), chunk.dtype)
    whole = lax.dynamic_update_slice_in_dim(whole, chunk, index * height, 0)
    for offset in range(1, size):
        got = partner_xor(chunk, axis, shift, offset)
        whole = lax.dynamic_update_slice_in_dim(whole, got, (index ^ offset) * height, 0)
    return whole


def axis_groups(axis, first):
    bits = lax.axis_size(axis).bit_length() - 1
    groups = []
    shift = first
    while shift < bits:
        width = min(2, bits - shift)
        groups.append((axis, shift, 2**width))
        shift += width
    return groups


def group_total(value, axis, shift, size):
    index = group_index(axis, shift, size)
    received = [value] + [partner_xor(value, axis, shift, offset) for offset in range(1, size)]
    ordered = []
    for slot in range(size):
        pick = received[0]
        for offset in range(1, size):
            pick = jnp.where((index ^ offset) == slot, received[offset], pick)
        ordered.append(pick)
    return functools.reduce(jnp.add, ordered)


def on_device(response):
    row_count = response.shape[0] * lax.axis_size("inner") * lax.axis_size("wide")
    bit = jnp.reshape(lax.axis_index("wide") & 1, (1,)).astype(jnp.int32)
    keep, send = gram_halves(response, row_count, bit)
    partial_sum = keep + partner_xor(send, "wide", 0, 1)
    groups = axis_groups("inner", 0) + axis_groups("wide", 1)
    for group in groups[:-1]:
        partial_sum = scatter_sum(partial_sum, *group)
    partial_sum = group_total(partial_sum, *groups[-1])
    for group in reversed(groups[:-1]):
        partial_sum = gather_all(partial_sum, *group)
    got = partner_xor(partial_sum, "wide", 0, 1)
    upper_factor, inverse_upper = cholesky_and_inverse(bit, partial_sum, got)
    q_rows = rows_times(response, inverse_upper)
    return (upper_factor, q_rows)


def solution(mesh):
    in_specs = (P(("inner", "wide"), None),)
    out_specs = (P(), P(("inner", "wide"), None))
    return jax.shard_map(
        on_device, mesh=mesh, in_specs=in_specs, out_specs=out_specs, check_vma=False
    )
```

```python
import functools

import jax
import jax.numpy as jnp
from jax import lax
from jax.experimental import pallas as pl
from jax.experimental.pallas import tpu as pltpu
from jax.sharding import PartitionSpec as P


BLOCK = 128
SLAB = 8


PAD = 32
STACK = 4 * BLOCK + PAD


def local_grid(size):
    return lax.broadcasted_iota(jnp.int32, (size, size), 0), lax.broadcasted_iota(jnp.int32, (size, size), 1)


def pack_pair(first, second):
    r, c = local_grid(first.shape[0])
    packed = jnp.where(r > c, first, second)
    diagonal = jnp.sum(jnp.where(r == c, first, 0.0), axis=0, keepdims=True)
    pad = jnp.concatenate([diagonal, jnp.zeros((PAD - 1, first.shape[0]), jnp.float32)], axis=0)
    return packed, pad


def unpack_pair(packed, diagonal):
    r, c = local_grid(packed.shape[0])
    flipped = packed.T
    first = jnp.where(r > c, packed, jnp.where(r == c, diagonal, flipped))
    second = jnp.where(r <= c, packed, flipped)
    return first, second


def lower_stacks(acc_ref):
    b = BLOCK
    p01, d0 = pack_pair(acc_ref[0:b, 0:b], acc_ref[b:2 * b, b:2 * b])
    p23, d2 = pack_pair(acc_ref[2 * b:3 * b, 2 * b:3 * b], acc_ref[3 * b:4 * b, 3 * b:4 * b])
    first = jnp.concatenate([acc_ref[b:4 * b, 0:b], p01, d0], axis=0)
    second = jnp.concatenate([acc_ref[2 * b:4 * b, b:2 * b], acc_ref[3 * b:4 * b, 2 * b:3 * b], p23, d2], axis=0)
    return first, second


def fill_gram(work_ref, first_ref, second_ref):
    b = BLOCK
    work_ref[b:4 * b, 0:b] = first_ref[0:3 * b, :]
    d0, d1 = unpack_pair(first_ref[3 * b:4 * b, :], first_ref[4 * b:4 * b + 1, :])
    work_ref[0:b, 0:b] = d0
    work_ref[b:2 * b, b:2 * b] = d1
    work_ref[2 * b:4 * b, b:2 * b] = second_ref[0:2 * b, :]
    work_ref[3 * b:4 * b, 2 * b:3 * b] = second_ref[2 * b:3 * b, :]
    d2, d3 = unpack_pair(second_ref[3 * b:4 * b, :], second_ref[4 * b:4 * b + 1, :])
    work_ref[2 * b:3 * b, 2 * b:3 * b] = d2
    work_ref[3 * b:4 * b, 3 * b:4 * b] = d3
    for i in range(4):
        for j in range(i + 1, 4):
            work_ref[i * b:(i + 1) * b, j * b:(j + 1) * b] = work_ref[j * b:(j + 1) * b, i * b:(i + 1) * b].T


def hdot(left, right):
    return jnp.dot(left, right, precision=lax.Precision.HIGHEST, preferred_element_type=jnp.float32)


def sweep_block(diag):
    size = diag.shape[0]
    eye = (lax.broadcasted_iota(jnp.int32, (size, size), 0) == lax.broadcasted_iota(jnp.int32, (size, size), 1)).astype(jnp.float32)
    joined = jnp.concatenate([diag, eye], axis=1)
    slabs = [joined[s * SLAB:(s + 1) * SLAB] for s in range(size // SLAB)]
    rows = lax.broadcasted_iota(jnp.int32, (SLAB, 1), 0)
    for j in range(size):
        s, t = divmod(j, SLAB)
        scale = lax.rsqrt(slabs[s][t:t + 1, j:j + 1])
        top = slabs[s][t:t + 1, :] * scale
        for q in range(s + 1, len(slabs)):
            slabs[q] = slabs[q] - (slabs[q][:, j:j + 1] * scale) * top
        here = slabs[s]
        updated = here - (here[:, j:j + 1] * scale) * top
        slabs[s] = jnp.where(rows > t, updated, jnp.where(rows == t, top, here))
    joined = jnp.concatenate(slabs, axis=0)
    r = lax.broadcasted_iota(jnp.int32, (size, size), 0)
    c = lax.broadcasted_iota(jnp.int32, (size, size), 1)
    return jnp.where(c >= r, joined[:, :size], 0.0), joined[:, size:]


def chol_kernel(bit_ref, mine_ref, got_ref, u_ref, uinv_ref, work_ref, aug_ref, inv_ref):
    n = u_ref.shape[0]

    @pl.when(bit_ref[0] == 0)
    def _():
        fill_gram(work_ref, mine_ref, got_ref)

    @pl.when(bit_ref[0] != 0)
    def _():
        fill_gram(work_ref, got_ref, mine_ref)

    aug_ref[...] = jnp.zeros_like(aug_ref)
    blocks = n // BLOCK
    for k in range(blocks):
        lo, hi = k * BLOCK, (k + 1) * BLOCK
        if hi < n:
            u_ref[hi:n, lo:hi] = jnp.zeros((n - hi, BLOCK), jnp.float32)
            uinv_ref[hi:n, lo:hi] = jnp.zeros((n - hi, BLOCK), jnp.float32)
        u_kk, inv_kk = sweep_block(work_ref[lo:hi, lo:hi])
        u_ref[lo:hi, lo:hi] = u_kk
        if k > 0:
            inv_row = hdot(inv_kk, aug_ref[lo:hi, 0:lo])
            inv_ref[lo:hi, 0:lo] = inv_row
            uinv_ref[0:lo, lo:hi] = inv_row.T
        inv_ref[lo:hi, lo:hi] = inv_kk
        uinv_ref[lo:hi, lo:hi] = inv_kk.T
        if hi < n:
            u_off = hdot(inv_kk, work_ref[lo:hi, hi:n])
            u_ref[lo:hi, hi:n] = u_off
            u_off_t = u_off.T
            work_ref[hi:n, hi:n] = work_ref[hi:n, hi:n] - hdot(u_off_t, u_off)
            aug_ref[hi:n, 0:hi] = aug_ref[hi:n, 0:hi] - hdot(u_off_t, inv_ref[lo:hi, 0:hi])


def cholesky_and_inverse(bit, mine, got):
    n = 4 * BLOCK
    spec = pl.BlockSpec(memory_space=pltpu.VMEM)
    return pl.pallas_call(
        chol_kernel,
        out_shape=(jax.ShapeDtypeStruct((n, n), jnp.float32), jax.ShapeDtypeStruct((n, n), jnp.float32)),
        in_specs=[pl.BlockSpec(memory_space=pltpu.SMEM), spec, spec],
        out_specs=(spec, spec),
        scratch_shapes=[pltpu.VMEM((n, n), jnp.float32) for _ in range(3)],
    )(bit, mine, got)


def rows_kernel(a_ref, w_ref, o_ref):
    width = w_ref.shape[1]
    half = width // 2
    o_ref[:, 0:half] = hdot(a_ref[:, 0:half], w_ref[0:half, 0:half])
    o_ref[:, half:width] = hdot(a_ref[...], w_ref[:, half:width])


def rows_times(matrix, weights):
    rows, width = matrix.shape
    tile = min(rows, 1024)
    return pl.pallas_call(
        rows_kernel,
        out_shape=jax.ShapeDtypeStruct((rows, weights.shape[1]), jnp.float32),
        grid=(rows // tile,),
        in_specs=[
            pl.BlockSpec((tile, width), lambda i: (i, 0)),
            pl.BlockSpec(weights.shape, lambda i: (0, 0)),
        ],
        out_specs=pl.BlockSpec((tile, weights.shape[1]), lambda i: (i, 0)),
    )(matrix, weights)


def matmul(left, right):
    return jnp.dot(left, right, precision=lax.Precision.HIGHEST, preferred_element_type=jnp.float32)


def cross(left, right):
    return lax.dot_general(
        left,
        right,
        (((0,), (0,)), ((), ())),
        precision=lax.Precision.HIGHEST,
        preferred_element_type=jnp.float32,
    )


def gram_kernel(row_count, bit_ref, a_ref, keep_ref, send_ref, acc_ref):
    step = pl.program_id(0)
    half = a_ref.shape[1] // 2

    @pl.when(step == 0)
    def _():
        acc_ref[...] = jnp.zeros_like(acc_ref)

    a = a_ref[...]
    acc_ref[:, 0:half] += cross(a, a[:, 0:half])
    acc_ref[half:, half:] += cross(a[:, half:], a[:, half:])

    @pl.when(step == pl.num_programs(0) - 1)
    def _():
        first, second = lower_stacks(acc_ref)
        first = first / row_count
        second = second / row_count

        @pl.when(bit_ref[0] == 0)
        def _():
            keep_ref[...] = first
            send_ref[...] = second

        @pl.when(bit_ref[0] != 0)
        def _():
            keep_ref[...] = second
            send_ref[...] = first


def gram_halves(matrix, row_count, bit):
    rows, width = matrix.shape
    tile = min(rows, 1024)
    half = jax.ShapeDtypeStruct((STACK, BLOCK), jnp.float32)
    return pl.pallas_call(
        functools.partial(gram_kernel, row_count),
        out_shape=(half, half),
        grid=(rows // tile,),
        in_specs=[
            pl.BlockSpec(memory_space=pltpu.SMEM),
            pl.BlockSpec((tile, width), lambda i: (i, 0)),
        ],
        out_specs=(
            pl.BlockSpec((STACK, BLOCK), lambda i: (0, 0)),
            pl.BlockSpec((STACK, BLOCK), lambda i: (0, 0)),
        ),
        scratch_shapes=[pltpu.VMEM((width, width), jnp.float32)],
    )(bit, matrix)


def group_index(axis, shift, size):
    return (lax.axis_index(axis) >> shift) & (size - 1)


def partner_xor(value, axis, shift, offset):
    mask = offset << shift
    pairs = [(source, source ^ mask) for source in range(lax.axis_size(axis))]
    return lax.ppermute(value, axis, pairs)


def scatter_sum(value, axis, shift, size):
    height = value.shape[0] // size
    index = group_index(axis, shift, size)
    chunk = lambda j: lax.dynamic_slice_in_dim(value, j * height, height, 0)
    total = chunk(index)
    for offset in range(1, size):
        total = total + partner_xor(chunk(index ^ offset), axis, shift, offset)
    return total


def gather_all(chunk, axis, shift, size):
    height = chunk.shape[0]
    index = group_index(axis, shift, size)
    whole = jnp.zeros((height * size, chunk.shape[1]), chunk.dtype)
    whole = lax.dynamic_update_slice_in_dim(whole, chunk, index * height, 0)
    for offset in range(1, size):
        got = partner_xor(chunk, axis, shift, offset)
        whole = lax.dynamic_update_slice_in_dim(whole, got, (index ^ offset) * height, 0)
    return whole


def axis_groups(axis, first):
    bits = lax.axis_size(axis).bit_length() - 1
    groups = []
    shift = first
    while shift < bits:
        width = min(2, bits - shift)
        groups.append((axis, shift, 2**width))
        shift += width
    return groups


def group_total(value, axis, shift, size):
    index = group_index(axis, shift, size)
    received = [value] + [partner_xor(value, axis, shift, offset) for offset in range(1, size)]
    ordered = []
    for slot in range(size):
        pick = received[0]
        for offset in range(1, size):
            pick = jnp.where((index ^ offset) == slot, received[offset], pick)
        ordered.append(pick)
    return functools.reduce(jnp.add, ordered)


def on_device(response):
    row_count = response.shape[0] * lax.axis_size("inner") * lax.axis_size("wide")
    bit = jnp.reshape(lax.axis_index("wide") & 1, (1,)).astype(jnp.int32)
    keep, send = gram_halves(response, row_count, bit)
    partial_sum = keep + partner_xor(send, "wide", 0, 1)
    groups = axis_groups("inner", 0) + axis_groups("wide", 1)
    for group in groups[:-1]:
        partial_sum = scatter_sum(partial_sum, *group)
    partial_sum = group_total(partial_sum, *groups[-1])
    for group in reversed(groups[:-1]):
        partial_sum = gather_all(partial_sum, *group)
    got = partner_xor(partial_sum, "wide", 0, 1)
    upper_factor, inverse_upper = cholesky_and_inverse(bit, partial_sum, got)
    q_rows = rows_times(response, inverse_upper)
    return (upper_factor, q_rows)


def solution(mesh):
    in_specs = (P(("inner", "wide"), None),)
    out_specs = (P(), P(("inner", "wide"), None))
    return jax.shard_map(
        on_device, mesh=mesh, in_specs=in_specs, out_specs=out_specs, check_vma=False
    )
```
